512 devices in a mesh: tm: 128 (over y, z, x_hi), series: 4 (over x_lo, core).
Axes of the slice: x: 4 (x_hi: 2, x_lo: 2; x = x_hi * 2 + x_lo), y: 8, z: 8, core: 2. Of those that a mesh axis runs over, the one named last changes fastest.
Arguments:
- returns: float32 [32768, 8192], P('tm', 'series'), may hold values from -40 to 40
- sector: int32 [8192], P('series'), may hold values from 0 to 511, as said below
Outputs:
- shrunk_variance: float32 [32768, 8192], P('tm', 'series')
The draws below stay inside these ranges and needn't reach their ends.
Inputs may be any that keep to these rules, and one draw needn't show every extreme that they name: `sector`: sectors differ widely in size; some sectors may hold no series.
All inputs are finite; a program needn't handle non-finite values.
Results may differ from the reference program's by a relative error of at most 0.0003.
Values sent between devices are 32-bit elements; how exact they have to be, the bound alone decides.
A program may use at most 64 MiB of HBM per device.

```python
import jax
import jax.numpy as jnp
from jax import lax

T_DEV = 256
W = 64
SECTORS = 512
STEPS = 32768
SERIES = 8192
N_TM = 128


def sector_labels(key):
    base = jax.random.fold_in(key, 1013)
    first = jax.random.randint(jax.random.fold_in(base, 1), (SERIES,), 0, SECTORS)
    second = jax.random.randint(jax.random.fold_in(base, 2), (SERIES,), 0, SECTORS)
    raw = first * second // SECTORS
    order = jax.random.permutation(jax.random.fold_in(base, 3), SECTORS)
    return order[raw].astype(jnp.int32)


def draw_sector(key, part):
    return sector_labels(key)


def draw_returns(key, part):
    labels = sector_labels(key)
    base = jax.random.fold_in(key, 2027)
    common = jax.random.normal(jax.random.fold_in(base, 1), (STEPS, SECTORS), jnp.float32)
    loading = jax.random.uniform(jax.random.fold_in(base, 2), (SERIES,), jnp.float32, 0.5, 1.5)
    volatility = jnp.exp(jax.random.uniform(jax.random.fold_in(base, 3), (SERIES,), jnp.float32, jnp.log(0.3), jnp.log(1.5)))
    position = jnp.arange(STEPS, dtype=jnp.float32) / STEPS
    noise = jax.random.normal(jax.random.fold_in(base, 4), (STEPS, SERIES), jnp.float32)
    trend = 1.0 + 2.0 * position
    values = trend[:, None] * (loading[None, :] * common[:, labels] + volatility[None, :] * noise)
    return jnp.clip(values, -40.0, 40.0).astype(jnp.float32)


def setup_inputs(seed: int = 0) -> dict:
    streams_of = jax.random.split(jax.random.key(seed), 3)
    return {
        "returns": draw_returns(jax.random.fold_in(streams_of[2], 71), 0),
        "sector": draw_sector(jax.random.fold_in(streams_of[2], 71), 0),
    }


ridge_rate = 0.05
shrink_weight = 0.3
highest = lax.Precision.HIGHEST


def sector_table(sector):
    labels = jnp.arange(SECTORS, dtype=jnp.int32)
    return (sector[:, None] == labels[None, :]).astype(jnp.float32)


def band_matrix(rows):
    row_pos = jnp.arange(rows, dtype=jnp.int32)[:, None]
    col_pos = jnp.arange(rows + W - 1, dtype=jnp.int32)[None, :]
    return ((col_pos >= row_pos) & (col_pos < row_pos + W)).astype(jnp.float32)


def window_variance(ext_returns, ext_factor, first_step):
    rows = ext_returns.shape[0] - (W - 1)
    series_width = ext_returns.shape[1]
    stacked = jnp.concatenate([ext_returns, ext_factor, ext_returns * ext_returns,
                               ext_factor * ext_factor, ext_returns * ext_factor], axis=1)
    moments = jnp.dot(band_matrix(rows), stacked, precision=highest, preferred_element_type=jnp.float32)
    sum_ret = moments[:, :series_width]
    sum_fac = moments[:, series_width:2 * series_width]
    sum_rr = moments[:, 2 * series_width:3 * series_width]
    sum_ff = moments[:, 3 * series_width:4 * series_width]
    sum_rf = moments[:, 4 * series_width:]
    steps_seen = jnp.minimum(first_step + jnp.arange(rows, dtype=jnp.int32) + 1, W).astype(jnp.float32)[:, None]
    centred_rr = sum_rr - sum_ret * sum_ret / steps_seen
    centred_ff = sum_ff - sum_fac * sum_fac / steps_seen
    centred_rf = sum_rf - sum_ret * sum_fac / steps_seen
    return (centred_rr - centred_rf * centred_rf / (centred_ff + ridge_rate * steps_seen)) / steps_seen


def reference(returns, sector):
    table = sector_table(sector)
    sums = jnp.dot(returns, table, precision=highest, preferred_element_type=jnp.float32)
    counts = jnp.sum(table, axis=0)
    means = sums / jnp.maximum(counts, 1.0)[None, :]
    factor = jnp.dot(means, table.T, precision=highest, preferred_element_type=jnp.float32)
    zeros = jnp.zeros((W - 1, SERIES), jnp.float32)
    padded_ret = jnp.concatenate([zeros, returns], axis=0)
    padded_fac = jnp.concatenate([zeros, factor], axis=0)

    def block(block_index):
        start = (block_index * T_DEV).astype(jnp.int32)
        ext_returns = lax.dynamic_slice_in_dim(padded_ret, start, T_DEV + W - 1, 0)
        ext_factor = lax.dynamic_slice_in_dim(padded_fac, start, T_DEV + W - 1, 0)
        return window_variance(ext_returns, ext_factor, start)

    variance = lax.map(block, jnp.arange(N_TM, dtype=jnp.int32)).reshape(STEPS, SERIES)
    totals = jnp.dot(jnp.sum(variance, axis=0)[None, :], table, precision=highest, preferred_element_type=jnp.float32)[0]
    sector_mean = totals / (STEPS * jnp.maximum(counts, 1.0))
    pooled = jnp.dot(sector_mean[None, :], table.T, precision=highest, preferred_element_type=jnp.float32)
    return (1.0 - shrink_weight) * variance + shrink_weight * pooled
```

```python
import jax
import jax.numpy as jnp
from jax import lax
from jax.experimental import pallas as pl
from jax.experimental.pallas import tpu as pltpu
from jax.sharding import Mesh
from jax.sharding import PartitionSpec as P

W = 64
SECTORS = 512
AXES = ("y", "z", "xh", "xl", "c")
MESH_IDS = pl.DeviceIdType.MESH

ridge_rate = 0.05
shrink_weight = 0.3

COUNT_ROWS = 8
CHUNK = 256
EARLY = 3


def split3(value):
    hi = value.astype(jnp.bfloat16)
    rest = value - hi.astype(jnp.float32)
    mid = rest.astype(jnp.bfloat16)
    lo = (rest - mid.astype(jnp.float32)).astype(jnp.bfloat16)
    return jnp.concatenate([hi, mid, lo], axis=0)


def joined3(value):
    rows = value.shape[0] // 3
    return value[:rows] + value[rows : 2 * rows] + value[2 * rows :]


def windowed(value):
    shift = 1
    while shift < W:
        value = value + pltpu.roll(value, shift, 0)
        shift *= 2
    return value[W:]


def window_variance(ret, fac, steps, inv_steps):
    sum_ret = windowed(ret)
    sum_fac = windowed(fac)
    sum_rr = windowed(ret * ret)
    sum_ff = windowed(fac * fac)
    sum_rf = windowed(ret * fac)
    mean_fac = sum_fac * inv_steps
    centred_rr = sum_rr - sum_ret * sum_ret * inv_steps
    centred_ff = sum_ff - sum_fac * mean_fac
    centred_rf = sum_rf - sum_ret * mean_fac
    return (
        centred_rr - centred_rf * centred_rf / (centred_ff + ridge_rate * steps)
    ) * inv_steps


def by_eights(value):
    total = value[0:8]
    for row in range(8, value.shape[0], 8):
        total = total + value[row : row + 8]
    return total


def remote(src, dst, send, recv, device):
    return pltpu.make_async_remote_copy(
        src_ref=src,
        dst_ref=dst,
        send_sem=send,
        recv_sem=recv,
        device_id=device,
        device_id_type=MESH_IDS,
    )


def make_kernel(sizes, time_rows, series):
    n_y, n_z = sizes["y"], sizes["z"]
    half = time_rows // 2
    chunks = series // CHUNK
    tail = W // 2

    def kernel(
        ret_hbm,
        sector_ref,
        var_hbm,
        pooled_ref,
        ret,
        fac,
        table,
        part,
        mine,
        from_core,
        from_pair,
        means,
        prior,
        var,
        col,
        gx,
        gy,
        gz,
        load_sem,
        halo_send,
        halo_recv,
        ex_send,
        ex_recv,
        pm_send,
        pm_recv,
        out_sem,
        gx_send,
        gx_recv,
        gy_send,
        gy_recv,
        gz_send,
        gz_recv,
    ):
        y, z = lax.axis_index("y"), lax.axis_index("z")
        xh, xl, c = lax.axis_index("xh"), lax.axis_index("xl"), lax.axis_index("c")
        block = (y * n_z + z) * 2 + xh
        n_blocks = n_y * n_z * 2

        def place(b):
            b = lax.rem(b + n_blocks, n_blocks)
            return {"y": b // (2 * n_z), "z": lax.rem(b // 2, n_z), "xh": lax.rem(b, 2)}

        following, previous = place(block + 1), place(block - 1)
        core = {"c": 1 - c}
        pair = {"xl": 1 - xl}

        def x_peer(d):
            p = lax.rem(xh * 4 + xl * 2 + c + d, 8)
            return {"xh": p // 4, "xl": lax.rem(p // 2, 2), "c": lax.rem(p, 2)}

        def y_peer(d):
            return {"y": lax.rem(y + d, n_y)}

        def z_peer(d):
            return {"z": lax.rem(z + d, n_z)}

        peers = [following, previous]
        peers += [x_peer(d) for d in range(1, 8)]
        peers += [y_peer(d) for d in range(1, n_y)]
        peers += [z_peer(d) for d in range(1, n_z)]
        barrier = pltpu.get_barrier_semaphore()
        for peer in peers:
            pl.semaphore_signal(barrier, inc=1, device_id=peer, device_id_type=MESH_IDS)

        loads = [
            pltpu.make_async_copy(
                ret_hbm.at[time_rows - W :], ret.at[time_rows:], load_sem.at[0]
            ),
            pltpu.make_async_copy(
                ret_hbm.at[: time_rows - W], ret.at[W:time_rows], load_sem.at[1]
            ),
        ]
        for load in loads:
            load.start()

        @pl.loop(0, chunks)
        def _(i):
            at = pl.multiple_of(i * CHUNK, CHUNK)
            labels = lax.broadcasted_iota(jnp.int32, (SECTORS, CHUNK), 0)
            hit = labels == sector_ref[:, pl.ds(at, CHUNK)]
            table[:, pl.ds(at, CHUNK)] = hit.astype(jnp.float32).astype(jnp.bfloat16)

        loads[0].wait()
        pl.semaphore_wait(barrier, len(peers))

        def halo(i):
            at = pl.multiple_of(i * CHUNK, CHUNK)
            return remote(
                ret.at[time_rows:, pl.ds(at, CHUNK)],
                ret.at[:W, pl.ds(at, CHUNK)],
                halo_send.at[i],
                halo_recv.at[i],
                following,
            )

        for i in range(EARLY):
            halo(i).start()
        loads[1].wait()

        def partial_sums(which, into):
            first = pl.multiple_of(W + which * half, W)
            into[...] = jnp.zeros_like(into)

            @pl.loop(0, chunks)
            def _(i):
                at = pl.multiple_of(i * CHUNK, CHUNK)
                lhs = jnp.concatenate(
                    [
                        split3(ret[pl.ds(first, half), pl.ds(at, CHUNK)]),
                        jnp.ones((2 * COUNT_ROWS, CHUNK), jnp.bfloat16),
                    ],
                    axis=0,
                )
                got = lax.dot_general(
                    lhs,
                    table[:, pl.ds(at, CHUNK)],
                    (((1,), (1,)), ((), ())),
                    preferred_element_type=jnp.float32,
                )
                into[:half] += joined3(got[: 3 * half])
                into[half:] += got[3 * half : 3 * half + COUNT_ROWS]

        partial_sums(1 - c, part)
        to_core = remote(part, from_core, ex_send.at[0], ex_recv.at[0], core)
        to_core.start()
        partial_sums(c, mine)
        to_core.wait_recv()
        mine[...] = mine[...] + from_core[...]
        to_pair = remote(mine, from_pair, ex_send.at[1], ex_recv.at[1], pair)
        to_pair.start()
        to_pair.wait_recv()
        for i in range(EARLY, chunks):
            halo(i).start()

        own = pl.ds(pl.multiple_of(c * half, half), half)
        counts = jnp.maximum(mine[half : half + 1] + from_pair[half : half + 1], 1.0)
        means[own] = (mine[:half] + from_pair[:half]) / counts
        share = remote(means.at[own], means.at[own], ex_send.at[2], ex_recv.at[2], core)
        share.start()
        share.wait_recv()

        low = pl.multiple_of(c * tail, tail)
        pm_rows = prior.at[pl.ds(low, tail)]
        pm_on = remote(
            means.at[pl.ds(time_rows - W + low, tail)],
            pm_rows,
            pm_send.at[0],
            pm_recv.at[0],
            following,
        )
        pm_on.start()

        full = jnp.float32(W)

        def out_copy(i, first, rows, slot):
            at = pl.multiple_of(i * CHUNK, CHUNK)
            return pltpu.make_async_copy(
                var.at[pl.ds(first, rows), pl.ds(at, CHUNK)],
                var_hbm.at[pl.ds(first, rows), pl.ds(at, CHUNK)],
                out_sem.at[slot, i],
            )

        @pl.loop(0, chunks)
        def _(i):
            at = pl.multiple_of(i * CHUNK, CHUNK)
            got = jnp.dot(
                split3(means[...]),
                table[:, pl.ds(at, CHUNK)],
                preferred_element_type=jnp.float32,
            )
            fac[pl.ds(W, time_rows), pl.ds(at, CHUNK)] = joined3(got)
            for s in range(CHUNK // 128):
                lanes = pl.ds(at + s * 128, 128)
                value = window_variance(
                    ret[pl.ds(W, time_rows), lanes],
                    fac[pl.ds(W, time_rows), lanes],
                    full,
                    1.0 / full,
                )
                col[:, lanes] = by_eights(value)
                var[pl.ds(W, time_rows - W), lanes] = (1.0 - shrink_weight) * value
            out_copy(i, W, time_rows - W, 0).start()

        pm_on.wait_recv()
        pm_share = remote(pm_rows, pm_rows, pm_send.at[1], pm_recv.at[1], core)
        pm_share.start()
        pm_share.wait_recv()
        started = block > 0

        @pl.loop(0, chunks)
        def _(i):
            at = pl.multiple_of(i * CHUNK, CHUNK)
            got = jnp.dot(
                split3(jnp.where(started, prior[...], 0.0)),
                table[:, pl.ds(at, CHUNK)],
                preferred_element_type=jnp.float32,
            )
            fac[pl.ds(0, W), pl.ds(at, CHUNK)] = joined3(got)

        seen = lax.broadcasted_iota(jnp.int32, (W, 128), 0) + 1 + block * time_rows
        steps = jnp.minimum(seen, W).astype(jnp.float32)
        inv_steps = 1.0 / steps
        gx[0] = jnp.zeros((8, SECTORS), jnp.float32)

        @pl.loop(0, chunks)
        def _(i):
            at = pl.multiple_of(i * CHUNK, CHUNK)
            halo(i).wait_recv()
            for s in range(CHUNK // 128):
                lanes = pl.ds(at + s * 128, 128)
                before = jnp.where(started, ret[pl.ds(0, W), lanes], 0.0)
                value = window_variance(
                    jnp.concatenate([before, ret[pl.ds(W, W), lanes]], axis=0),
                    fac[pl.ds(0, 2 * W), lanes],
                    steps,
                    inv_steps,
                )
                col[:, lanes] += by_eights(value)
                var[pl.ds(0, W), lanes] = (1.0 - shrink_weight) * value
            out_copy(i, 0, W, 1).start()
            got = lax.dot_general(
                split3(col[:, pl.ds(at, CHUNK)]),
                table[:, pl.ds(at, CHUNK)],
                (((1,), (1,)), ((), ())),
                preferred_element_type=jnp.float32,
            )
            gx[0] += joined3(got)

        def exchange(buf, peer_of, send, recv, count, total):
            buf[0] = jnp.broadcast_to(total, (8, SECTORS))
            copies = [
                remote(
                    buf.at[0, pl.ds(0, 1)],
                    buf.at[d, pl.ds(0, 1)],
                    send.at[d],
                    recv.at[d],
                    peer_of(d),
                )
                for d in range(1, count)
            ]
            for copy in copies:
                copy.start()
            for copy in copies:
                copy.wait_recv()
            total = buf[0, 0:1]
            for d in range(1, count):
                total = total + buf[d, 0:1]
            for copy in copies:
                copy.wait_send()
            return total

        total = jnp.sum(gx[0], axis=0, keepdims=True)
        total = exchange(gx, x_peer, gx_send, gx_recv, 8, total)
        total = exchange(gy, y_peer, gy_send, gy_recv, n_y, total)
        total = exchange(gz, z_peer, gz_send, gz_recv, n_z, total)

        all_steps = float(time_rows * n_blocks)
        sector_mean = total / (all_steps * counts)
        got = jnp.dot(
            split3(jnp.broadcast_to(shrink_weight * sector_mean, (8, SECTORS))),
            table[...],
            preferred_element_type=jnp.float32,
        )
        pooled_ref[...] = joined3(got)[0:1]

        for i in range(chunks):
            out_copy(i, W, time_rows - W, 0).wait()
            out_copy(i, 0, W, 1).wait()
            halo(i).wait_send()
        for copy in (to_core, to_pair, share, pm_on, pm_share):
            copy.wait_send()

    return kernel


def solution(mesh):
    series_axis = mesh.shape["series"]
    torus = Mesh(mesh.devices.reshape(8, 8, 2, series_axis // 2, 2), AXES)
    sizes = dict(torus.shape)
    n_y, n_z = sizes["y"], sizes["z"]

    def local(returns, sector):
        time_rows, series = returns.shape
        half = time_rows // 2
        chunks = series // CHUNK
        f32 = jnp.float32
        dma = pltpu.SemaphoreType.DMA
        variance, pooled = pl.pallas_call(
            make_kernel(sizes, time_rows, series),
            name="rolling",
            out_shape=(
                jax.ShapeDtypeStruct((time_rows, series), f32),
                jax.ShapeDtypeStruct((1, series), f32),
            ),
            in_specs=[
                pl.BlockSpec(memory_space=pl.ANY),
                pl.BlockSpec(memory_space=pltpu.VMEM),
            ],
            out_specs=(
                pl.BlockSpec(memory_space=pl.ANY),
                pl.BlockSpec(memory_space=pltpu.VMEM),
            ),
            scratch_shapes=[
                pltpu.VMEM((time_rows + W, series), f32),
                pltpu.VMEM((time_rows + W, series), f32),
                pltpu.VMEM((SECTORS, series), jnp.bfloat16),
                pltpu.VMEM((half + COUNT_ROWS, SECTORS), f32),
                pltpu.VMEM((half + COUNT_ROWS, SECTORS), f32),
                pltpu.VMEM((half + COUNT_ROWS, SECTORS), f32),
                pltpu.VMEM((half + COUNT_ROWS, SECTORS), f32),
                pltpu.VMEM((time_rows, SECTORS), f32),
                pltpu.VMEM((W, SECTORS), f32),
                pltpu.VMEM((time_rows, series), f32),
                pltpu.VMEM((8, series), f32),
                pltpu.VMEM((8, 8, SECTORS), f32),
                pltpu.VMEM((n_y, 8, SECTORS), f32),
                pltpu.VMEM((n_z, 8, SECTORS), f32),
                dma((2,)),
                dma((chunks,)),
                dma((chunks,)),
                dma((3,)),
                dma((3,)),
                dma((2,)),
                dma((2,)),
                dma((2, chunks)),
                dma((8,)),
                dma((8,)),
                dma((n_y,)),
                dma((n_y,)),
                dma((n_z,)),
                dma((n_z,)),
            ],
            compiler_params=pltpu.CompilerParams(
                collective_id=0, has_side_effects=True, vmem_limit_bytes=56 * 2**20
            ),
        )(returns, sector[None, :])
        return variance + pooled

    return jax.shard_map(
        local,
        mesh=torus,
        in_specs=(P(("y", "z", "xh"), ("xl", "c")), P(("xl", "c"))),
        out_specs=P(("y", "z", "xh"), ("xl", "c")),
        check_vma=False,
    )
```

```python
import jax
import jax.numpy as jnp
from jax import lax
from jax.experimental import pallas as pl
from jax.experimental.pallas import tpu as pltpu
from jax.sharding import Mesh
from jax.sharding import PartitionSpec as P

W = 64
SECTORS = 512
AXES = ("y", "z", "xh", "xl", "c")
MESH_IDS = pl.DeviceIdType.MESH

ridge_rate = 0.05
shrink_weight = 0.3

LANES = 128
COUNT_ROWS = 8
CHUNK = 256
GROUPS = CHUNK // LANES
DEPTH = 512
KEPT = 3
PARTS = 2
EARLY = 2
MIDDLE = 4


def split3(value):
    hi = value.astype(jnp.bfloat16)
    rest = value - hi.astype(jnp.float32)
    mid = rest.astype(jnp.bfloat16)
    lo = (rest - mid.astype(jnp.float32)).astype(jnp.bfloat16)
    return hi, mid, lo


def split2(value):
    hi = value.astype(jnp.bfloat16)
    return hi, (value - hi.astype(jnp.float32)).astype(jnp.bfloat16)


def nn(a, b):
    return jnp.dot(a, b, preferred_element_type=jnp.float32)


def nt(a, b):
    return lax.dot_general(
        a, b, (((1,), (1,)), ((), ())), preferred_element_type=jnp.float32
    )


def eight(q):
    return pl.ds(8 * q, 8)


def spread(tile, run, pitch=8):
    per = run // 8
    return pl.ds(8 * pitch * (tile % per) + tile // per, 8, stride=pitch)


def kept(q, k):
    return pl.ds(KEPT * 8 * q + 8 * k, 8)


def carried(total, back):
    out = pltpu.roll(total, 1, 0)
    for j in range(2, back + 1):
        out = out + pltpu.roll(total, j, 0)
    return out


def totals_of(terms, run):
    total = terms(0)
    for q in range(1, run):
        total = [a + b for a, b in zip(total, terms(q))]
    return total


def slide(windows, terms, back):
    return [s + (v - pltpu.roll(v, back, 0)) for s, v in zip(windows, terms)]


def remote(src, dst, send, recv, device):
    return pltpu.make_async_remote_copy(
        src_ref=src,
        dst_ref=dst,
        send_sem=send,
        recv_sem=recv,
        device_id=device,
        device_id_type=MESH_IDS,
    )


def make_kernel(sizes, time_rows, series):
    n_y, n_z = sizes["y"], sizes["z"]
    half = time_rows // 2
    chunks = series // CHUNK
    tail = W // 2
    run = time_rows // 8
    back = W // run
    edge = 2 * W
    edge_run = edge // 8
    edge_back = W // edge_run

    def kernel(
        ret_hbm,
        sector_hbm,
        var,
        pooled_ref,
        sector,
        ret,
        keep,
        table,
        part,
        mine,
        from_core,
        from_pair,
        means,
        prior,
        spreader,
        mean_parts,
        edge_parts,
        fac_a,
        fac_b,
        fac_edge,
        work,
        ret_edge,
        edge_steps,
        col,
        sums,
        gx,
        gy,
        gz,
        load_sem,
        halo_send,
        halo_recv,
        ex_send,
        ex_recv,
        pm_send,
        pm_recv,
        gx_send,
        gx_recv,
        gy_send,
        gy_recv,
        gz_send,
        gz_recv,
    ):
        loads = [
            pltpu.make_async_copy(sector_hbm, sector, load_sem.at[2]),
            pltpu.make_async_copy(
                ret_hbm.at[time_rows - W :], ret.at[time_rows:], load_sem.at[0]
            ),
            pltpu.make_async_copy(
                ret_hbm.at[: time_rows - W], ret.at[W:time_rows], load_sem.at[1]
            ),
        ]
        for load in loads:
            load.start()

        y, z = lax.axis_index("y"), lax.axis_index("z")
        xh, xl, c = lax.axis_index("xh"), lax.axis_index("xl"), lax.axis_index("c")
        block = (y * n_z + z) * 2 + xh
        n_blocks = n_y * n_z * 2

        def place(b):
            b = lax.rem(b + n_blocks, n_blocks)
            return {"y": b // (2 * n_z), "z": lax.rem(b // 2, n_z), "xh": lax.rem(b, 2)}

        following, previous = place(block + 1), place(block - 1)
        core = {"c": 1 - c}
        pair = {"xl": 1 - xl}

        def x_peer(d):
            p = lax.rem(xh * 4 + xl * 2 + c + d, 8)
            return {"xh": p // 4, "xl": lax.rem(p // 2, 2), "c": lax.rem(p, 2)}

        def y_peer(d):
            return {"y": lax.rem(y + d, n_y)}

        def z_peer(d):
            return {"z": lax.rem(z + d, n_z)}

        peers = [following, previous]
        peers += [x_peer(d) for d in range(1, 8)]
        peers += [y_peer(d) for d in range(1, n_y)]
        peers += [z_peer(d) for d in range(1, n_z)]
        barrier = pltpu.get_barrier_semaphore()
        for peer in peers:
            pl.semaphore_signal(barrier, inc=1, device_id=peer, device_id_type=MESH_IDS)

        loads[0].wait()

        @pl.loop(0, chunks)
        def _(i):
            at = pl.multiple_of(i * CHUNK, CHUNK)
            labels = lax.broadcasted_iota(jnp.int32, (SECTORS, CHUNK), 0)
            hit = labels == sector[:, pl.ds(at, CHUNK)]
            table[:, pl.ds(at, CHUNK)] = hit.astype(jnp.float32).astype(jnp.bfloat16)

        loads[1].wait()
        pl.semaphore_wait(barrier, len(peers))

        def halo(i):
            at = pl.multiple_of(i * CHUNK, CHUNK)
            return remote(
                ret.at[time_rows:, pl.ds(at, CHUNK)],
                ret.at[:W, pl.ds(at, CHUNK)],
                halo_send.at[i],
                halo_recv.at[i],
                following,
            )

        for i in range(EARLY):
            halo(i).start()
        loads[2].wait()

        def columns(h):
            return pl.ds(h * (SECTORS // PARTS), SECTORS // PARTS)

        def partial_sums(which, into, h):
            first = pl.multiple_of(W + which * half, W)
            into[h] = jnp.zeros(into.shape[1:], jnp.float32)

            @pl.loop(0, series // DEPTH)
            def _(i):
                cols = pl.ds(pl.multiple_of(i * DEPTH, DEPTH), DEPTH)
                hi, lo = split2(ret[pl.ds(first, half), cols])
                ones = jnp.ones((2 * COUNT_ROWS, DEPTH), jnp.bfloat16)
                got = nt(jnp.concatenate([hi, lo, ones], axis=0), table[columns(h), cols])
                into[h, :half] += got[:half] + got[half : 2 * half]
                into[h, half:] += got[2 * half : 2 * half + COUNT_ROWS]

        to_core = [
            remote(part.at[h], from_core.at[h], ex_send.at[0, h], ex_recv.at[0, h], core)
            for h in range(PARTS)
        ]
        to_pair = [
            remote(mine.at[h], from_pair.at[h], ex_send.at[1, h], ex_recv.at[1, h], pair)
            for h in range(PARTS)
        ]
        for h in range(PARTS):
            partial_sums(1 - c, part, h)
            to_core[h].start()
        for h in range(PARTS):
            partial_sums(c, mine, h)
            to_core[h].wait_recv()
            mine[h] = mine[h] + from_core[h]
            to_pair[h].start()
        for i in range(EARLY, MIDDLE):
            halo(i).start()

        full = float(W)

        @pl.loop(0, series // LANES)
        def _(g):
            lanes = pl.ds(pl.multiple_of(g * LANES, LANES), LANES)
            for tile in range(time_rows // 8):
                keep[g, spread(tile, run, 8 * KEPT), :] = ret[
                    pl.ds(W + 8 * tile, 8), lanes
                ]

            def terms(q):
                r = keep[g, kept(q, 0), :]
                return [r, r * r]

            windows = [carried(t, back) for t in totals_of(terms, run)]
            for q in range(run):
                windows = slide(windows, terms(q), back)
                keep[g, kept(q, 1), :] = windows[0]
                keep[g, kept(q, 2), :] = windows[1] - windows[0] * (
                    windows[0] * (1.0 / full)
                )

        place_in = lax.broadcasted_iota(jnp.int32, (8, LANES), 0)
        for q in range(edge_run):
            seen = (place_in - edge_back) * edge_run + q + 1 + block * time_rows
            steps = jnp.minimum(jnp.maximum(seen, 1), W).astype(jnp.float32)
            edge_steps[0, eight(q), :] = 1.0 / steps
            edge_steps[1, eight(q), :] = ridge_rate * steps

        own = pl.ds(pl.multiple_of(c * half, half), half)
        share = [
            remote(
                means.at[own, columns(h)],
                means.at[own, columns(h)],
                ex_send.at[2, h],
                ex_recv.at[2, h],
                core,
            )
            for h in range(PARTS)
        ]
        counts = []
        for h in range(PARTS):
            to_pair[h].wait_recv()
            both = mine[h] + from_pair[h]
            counts.append(jnp.maximum(both[half : half + 1], 1.0))
            means[own, columns(h)] = both[:half] * (1.0 / counts[h])
            share[h].start()
        counts = jnp.concatenate(counts, axis=1)
        for h in range(PARTS):
            share[h].wait_recv()

        low = pl.multiple_of(c * tail, tail)
        pm_rows = prior.at[pl.ds(low, tail)]
        pm_on = remote(
            means.at[pl.ds(time_rows - W + low, tail)],
            pm_rows,
            pm_send.at[0],
            pm_recv.at[0],
            following,
        )
        pm_on.start()
        for i in range(MIDDLE, chunks):
            halo(i).start()

        for j in range(SECTORS // LANES):
            lanes = pl.ds(j * LANES, LANES)
            for tile in range(time_rows // 8):
                spreader[j, spread(tile, run), :] = means[eight(tile), lanes]
            for k, value in enumerate(split2(spreader[j])):
                mean_parts[k, :, lanes] = value

        def gathered(parts, i):
            hot = table[:, pl.ds(pl.multiple_of(i * CHUNK, CHUNK), CHUNK)]
            return nn(parts[0], hot) + nn(parts[1], hot)

        def interior(i, fac):
            for s in range(GROUPS):
                g = i * GROUPS + s
                lanes = pl.ds(pl.multiple_of(g * LANES, LANES), LANES)
                inner = pl.ds(s * LANES, LANES)

                def terms(q):
                    f = fac[eight(q), inner]
                    return [f, f * f, keep[g, kept(q, 0), :] * f]

                windows = [carried(t, back) for t in totals_of(terms, run)]
                total = jnp.zeros((8, LANES), jnp.float32)
                for q in range(run):
                    windows = slide(windows, terms(q), back)
                    mean_fac = windows[0] * (1.0 / full)
                    cff = windows[1] - windows[0] * mean_fac
                    crf = windows[2] - keep[g, kept(q, 1), :] * mean_fac
                    value = (
                        keep[g, kept(q, 2), :] - crf * crf / (cff + ridge_rate * full)
                    ) * (1.0 / full)
                    total = total + value
                    work[s, eight(q), :] = (1.0 - shrink_weight) * value
                col[:, lanes] = jnp.where(place_in >= back, total, 0.0)
                for tile in range(W // 8, time_rows // 8):
                    var[eight(tile), lanes] = work[s, spread(tile, run), :]

        fac_a[...] = gathered(mean_parts, 0)

        def two_chunks(j):
            fac_b[...] = gathered(mean_parts, 2 * j + 1)
            interior(2 * j, fac_a)
            fac_a[...] = gathered(mean_parts, lax.rem(2 * j + 2, chunks))
            interior(2 * j + 1, fac_b)

        pl.loop(0, chunks // 2 - 1)(two_chunks)
        pm_on.wait_recv()
        pm_share = remote(pm_rows, pm_rows, pm_send.at[1], pm_recv.at[1], core)
        pm_share.start()
        two_chunks(chunks // 2 - 1)
        pm_share.wait_recv()
        started = block > 0

        for j in range(SECTORS // LANES):
            lanes = pl.ds(j * LANES, LANES)
            for tile in range(edge // 8):
                if tile < W // 8:
                    value = jnp.where(started, prior[eight(tile), lanes], 0.0)
                else:
                    value = means[eight(tile - W // 8), lanes]
                spreader[j, spread(tile, edge_run), :] = value
            for k, value in enumerate(split2(spreader[j, :edge, :])):
                edge_parts[k, :, lanes] = value

        @pl.loop(0, chunks)
        def _(i):
            fac_edge[i] = gathered(edge_parts, i)

        late = place_in >= edge_back
        sums[...] = jnp.zeros_like(sums)

        @pl.loop(0, chunks)
        def _(i):
            halo(i).wait_recv()
            for s in range(GROUPS):
                lanes = pl.ds(pl.multiple_of(i * CHUNK + s * LANES, LANES), LANES)
                inner = pl.ds(s * LANES, LANES)
                for tile in range(edge // 8):
                    value = ret[eight(tile), lanes]
                    if tile < W // 8:
                        value = jnp.where(started, value, 0.0)
                    ret_edge[s, spread(tile, edge_run), :] = value

                def terms(q):
                    f = fac_edge[i, eight(q), inner]
                    r = ret_edge[s, eight(q), :]
                    return [r, r * r, f, f * f, r * f]

                windows = [carried(t, edge_back) for t in totals_of(terms, edge_run)]
                total = jnp.zeros((8, LANES), jnp.float32)
                for q in range(edge_run):
                    windows = slide(windows, terms(q), edge_back)
                    inv = edge_steps[0, eight(q), :]
                    s_r, s_rr, s_f, s_ff, s_rf = windows
                    mean_fac = s_f * inv
                    cff = s_ff - s_f * mean_fac
                    crf = s_rf - s_r * mean_fac
                    value = (
                        (s_rr - s_r * (s_r * inv))
                        - crf * crf / (cff + edge_steps[1, eight(q), :])
                    ) * inv
                    total = total + value
                    work[s, eight(q), :] = (1.0 - shrink_weight) * value
                col[:, lanes] += jnp.where(late, total, 0.0)
                for tile in range(W // 8, edge // 8):
                    var[eight(tile - W // 8), lanes] = work[s, spread(tile, edge_run), :]
            cols = pl.ds(pl.multiple_of(i * CHUNK, CHUNK), CHUNK)
            hot = table[:, cols]
            got = nt(jnp.concatenate(split3(col[:, cols]), axis=0), hot)
            sums[...] += got[0:8] + got[8:16] + got[16:24]

        def exchange(buf, peer_of, send, recv, count, total):
            buf[0] = jnp.broadcast_to(total, (8, SECTORS))
            copies = [
                remote(
                    buf.at[0, pl.ds(0, 1)],
                    buf.at[d, pl.ds(0, 1)],
                    send.at[d],
                    recv.at[d],
                    peer_of(d),
                )
                for d in range(1, count)
            ]
            for copy in copies:
                copy.start()
            for copy in copies:
                copy.wait_recv()
            total = buf[0, 0:1]
            for d in range(1, count):
                total = total + buf[d, 0:1]
            return total, copies

        total = jnp.sum(sums[...], axis=0, keepdims=True)
        total, x_copies = exchange(gx, x_peer, gx_send, gx_recv, 8, total)
        total, y_copies = exchange(gy, y_peer, gy_send, gy_recv, n_y, total)
        total, z_copies = exchange(gz, z_peer, gz_send, gz_recv, n_z, total)

        all_steps = float(time_rows * n_blocks)
        sector_mean = total / (all_steps * counts)
        parts = split3(jnp.broadcast_to(shrink_weight * sector_mean, (8, SECTORS)))
        got = nn(jnp.concatenate(parts, axis=0), table[...])
        pooled_ref[...] = got[0:1] + got[8:9] + got[16:17]

        for i in range(chunks):
            halo(i).wait_send()
        for copy in (*to_core, *to_pair, *share, pm_on, pm_share):
            copy.wait_send()
        for copy in x_copies + y_copies + z_copies:
            copy.wait_send()

    return kernel


def last_add(var, pooled, out, held, sems):
    rows = var.shape[0] // 4
    copies = []
    for i in range(4):
        block = pl.ds(i * rows, rows)
        held[block] = var[block] + pooled[...]
        copies.append(pltpu.make_async_copy(held.at[block], out.at[block], sems.at[i]))
        copies[-1].start()
    for copy in copies:
        copy.wait()


def solution(mesh):
    series_axis = mesh.shape["series"]
    torus = Mesh(mesh.devices.reshape(8, 8, 2, series_axis // 2, 2), AXES)
    sizes = dict(torus.shape)
    n_y, n_z = sizes["y"], sizes["z"]

    def local(returns, sector):
        time_rows, series = returns.shape
        half = time_rows // 2
        chunks = series // CHUNK
        groups = series // LANES
        f32, bf16 = jnp.float32, jnp.bfloat16
        dma = pltpu.SemaphoreType.DMA
        vmem = pltpu.VMEM
        variance, pooled = pl.pallas_call(
            make_kernel(sizes, time_rows, series),
            name="rolling",
            out_shape=(
                vmem((time_rows, series), f32),
                vmem((1, series), f32),
            ),
            in_specs=[pl.BlockSpec(memory_space=pltpu.HBM)] * 2,
            out_specs=(
                pl.BlockSpec(memory_space=pltpu.VMEM),
                pl.BlockSpec(memory_space=pltpu.VMEM),
            ),
            scratch_shapes=[
                vmem((1, series), jnp.int32),
                vmem((time_rows + W, series), f32),
                vmem((groups, KEPT * time_rows, LANES), f32),
                vmem((SECTORS, series), bf16),
                vmem((PARTS, half + COUNT_ROWS, SECTORS // PARTS), f32),
                vmem((PARTS, half + COUNT_ROWS, SECTORS // PARTS), f32),
                vmem((PARTS, half + COUNT_ROWS, SECTORS // PARTS), f32),
                vmem((PARTS, half + COUNT_ROWS, SECTORS // PARTS), f32),
                vmem((time_rows, SECTORS), f32),
                vmem((W, SECTORS), f32),
                vmem((SECTORS // LANES, time_rows, LANES), f32),
                vmem((2, time_rows, SECTORS), bf16),
                vmem((2, 2 * W, SECTORS), bf16),
                vmem((time_rows, CHUNK), f32),
                vmem((time_rows, CHUNK), f32),
                vmem((chunks, 2 * W, CHUNK), f32),
                vmem((GROUPS, time_rows, LANES), f32),
                vmem((GROUPS, 2 * W, LANES), f32),
                vmem((2, 2 * W, LANES), f32),
                vmem((8, series), f32),
                vmem((8, SECTORS), f32),
                vmem((8, 8, SECTORS), f32),
                vmem((n_y, 8, SECTORS), f32),
                vmem((n_z, 8, SECTORS), f32),
                dma((3,)),
                dma((chunks,)),
                dma((chunks,)),
                dma((3, PARTS)),
                dma((3, PARTS)),
                dma((2,)),
                dma((2,)),
                dma((8,)),
                dma((8,)),
                dma((n_y,)),
                dma((n_y,)),
                dma((n_z,)),
                dma((n_z,)),
            ],
            compiler_params=pltpu.CompilerParams(
                collective_id=0, has_side_effects=True, vmem_limit_bytes=48 * 2**20
            ),
        )(
            pltpu.with_memory_space_constraint(returns, pltpu.HBM),
            pltpu.with_memory_space_constraint(sector[None, :], pltpu.HBM),
        )
        return pl.pallas_call(
            last_add,
            name="last_add",
            out_shape=jax.ShapeDtypeStruct((time_rows, series), f32),
            in_specs=[pl.BlockSpec(memory_space=pltpu.VMEM)] * 2,
            out_specs=pl.BlockSpec(memory_space=pl.ANY),
            scratch_shapes=[vmem((time_rows, series), f32), dma((4,))],
            compiler_params=pltpu.CompilerParams(vmem_limit_bytes=8 * 2**20),
        )(variance, pooled)

    return jax.shard_map(
        local,
        mesh=torus,
        in_specs=(P(("y", "z", "xh"), ("xl", "c")), P(("xl", "c"))),
        out_specs=P(("y", "z", "xh"), ("xl", "c")),
        check_vma=False,
    )
```

```python
import jax
import jax.numpy as jnp
from jax import lax
from jax.experimental import pallas as pl
from jax.experimental.pallas import tpu as pltpu
from jax.sharding import Mesh
from jax.sharding import PartitionSpec as P

W = 64
SECTORS = 512
AXES = ("y", "z", "xh", "xl", "c")
MESH_IDS = pl.DeviceIdType.MESH

ridge_rate = 0.05
shrink_weight = 0.3

LANES = 128
COUNT_ROWS = 8
CHUNK = 256
GROUPS = CHUNK // LANES
DEPTH = 512
KEPT = 3
PARTS = 2
EARLY = 2
MIDDLE = 4
BATCH = 4
LAST = 2


def split3(value):
    hi = value.astype(jnp.bfloat16)
    rest = value - hi.astype(jnp.float32)
    mid = rest.astype(jnp.bfloat16)
    lo = (rest - mid.astype(jnp.float32)).astype(jnp.bfloat16)
    return hi, mid, lo


def split2(value):
    hi = value.astype(jnp.bfloat16)
    return hi, (value - hi.astype(jnp.float32)).astype(jnp.bfloat16)


def nn(a, b):
    return jnp.dot(a, b, preferred_element_type=jnp.float32)


def nt(a, b):
    return lax.dot_general(
        a, b, (((1,), (1,)), ((), ())), preferred_element_type=jnp.float32
    )


def eight(q):
    return pl.ds(8 * q, 8)


def spread(tile, run, pitch=8):
    per = run // 8
    return pl.ds(8 * pitch * (tile % per) + tile // per, 8, stride=pitch)


def kept(q, k):
    return pl.ds(KEPT * 8 * q + 8 * k, 8)


def carried(total, back):
    out = pltpu.roll(total, 1, 0)
    for j in range(2, back + 1):
        out = out + pltpu.roll(total, j, 0)
    return out


def totals_of(terms, run):
    total = terms(0)
    for q in range(1, run):
        total = [a + b for a, b in zip(total, terms(q))]
    return total


def slide(windows, terms, back):
    return [s + (v - pltpu.roll(v, back, 0)) for s, v in zip(windows, terms)]


def remote(src, dst, send, recv, device):
    return pltpu.make_async_remote_copy(
        src_ref=src,
        dst_ref=dst,
        send_sem=send,
        recv_sem=recv,
        device_id=device,
        device_id_type=MESH_IDS,
    )


def make_kernel(sizes, time_rows, series):
    n_y, n_z = sizes["y"], sizes["z"]
    half = time_rows // 2
    chunks = series // CHUNK
    tail = W // 2
    run = time_rows // 8
    back = W // run
    edge = 2 * W
    edge_run = edge // 8
    edge_back = W // edge_run

    def kernel(
        ret_hbm,
        sector_hbm,
        var,
        pooled_ref,
        sector,
        ret,
        keep,
        table,
        part,
        mine,
        from_core,
        from_pair,
        means,
        prior,
        spreader,
        mean_parts,
        edge_parts,
        fac,
        fac_edge,
        work,
        ret_edge,
        edge_steps,
        col,
        sums,
        gx,
        gy,
        gz,
        load_sem,
        halo_send,
        halo_recv,
        ex_send,
        ex_recv,
        pm_send,
        pm_recv,
        gx_send,
        gx_recv,
        gy_send,
        gy_recv,
        gz_send,
        gz_recv,
    ):
        loads = [
            pltpu.make_async_copy(sector_hbm, sector, load_sem.at[2]),
            pltpu.make_async_copy(
                ret_hbm.at[time_rows - W :], ret.at[time_rows:], load_sem.at[0]
            ),
            pltpu.make_async_copy(
                ret_hbm.at[: time_rows - W], ret.at[W:time_rows], load_sem.at[1]
            ),
        ]
        for load in loads:
            load.start()

        y, z = lax.axis_index("y"), lax.axis_index("z")
        xh, xl, c = lax.axis_index("xh"), lax.axis_index("xl"), lax.axis_index("c")
        block = (y * n_z + z) * 2 + xh
        n_blocks = n_y * n_z * 2

        def place(b):
            b = lax.rem(b + n_blocks, n_blocks)
            return {"y": b // (2 * n_z), "z": lax.rem(b // 2, n_z), "xh": lax.rem(b, 2)}

        following, previous = place(block + 1), place(block - 1)
        core = {"c": 1 - c}
        pair = {"xl": 1 - xl}

        def x_peer(d):
            p = lax.rem(xh * 4 + xl * 2 + c + d, 8)
            return {"xh": p // 4, "xl": lax.rem(p // 2, 2), "c": lax.rem(p, 2)}

        def y_peer(d):
            return {"y": lax.rem(y + d, n_y)}

        def z_peer(d):
            return {"z": lax.rem(z + d, n_z)}

        peers = [following, previous]
        peers += [x_peer(d) for d in range(1, 8)]
        peers += [y_peer(d) for d in range(1, n_y)]
        peers += [z_peer(d) for d in range(1, n_z)]
        barrier = pltpu.get_barrier_semaphore()
        for peer in peers:
            pl.semaphore_signal(barrier, inc=1, device_id=peer, device_id_type=MESH_IDS)

        loads[0].wait()

        @pl.loop(0, chunks)
        def _(i):
            at = pl.multiple_of(i * CHUNK, CHUNK)
            labels = lax.broadcasted_iota(jnp.int32, (SECTORS, CHUNK), 0)
            hit = labels == sector[:, pl.ds(at, CHUNK)]
            table[:, pl.ds(at, CHUNK)] = hit.astype(jnp.float32).astype(jnp.bfloat16)

        loads[1].wait()
        pl.semaphore_wait(barrier, len(peers))

        def halo(i):
            at = pl.multiple_of(i * CHUNK, CHUNK)
            return remote(
                ret.at[time_rows:, pl.ds(at, CHUNK)],
                ret.at[:W, pl.ds(at, CHUNK)],
                halo_send.at[i],
                halo_recv.at[i],
                following,
            )

        for i in range(EARLY):
            halo(i).start()
        loads[2].wait()

        def columns(h):
            return pl.ds(h * (SECTORS // PARTS), SECTORS // PARTS)

        def partial_sums(which, into, h):
            first = pl.multiple_of(W + which * half, W)
            ones = jnp.ones((2 * COUNT_ROWS, DEPTH), jnp.bfloat16)
            got = None
            for at in range(0, series, DEPTH):
                cols = pl.ds(at, DEPTH)
                hi, lo = split2(ret[pl.ds(first, half), cols])
                more = nt(jnp.concatenate([hi, lo, ones], axis=0), table[columns(h), cols])
                got = more if got is None else got + more
            into[h, :half] = got[:half] + got[half : 2 * half]
            into[h, half:] = got[2 * half : 2 * half + COUNT_ROWS]

        to_core = [
            remote(part.at[h], from_core.at[h], ex_send.at[0, h], ex_recv.at[0, h], core)
            for h in range(PARTS)
        ]
        to_pair = [
            remote(mine.at[h], from_pair.at[h], ex_send.at[1, h], ex_recv.at[1, h], pair)
            for h in range(PARTS)
        ]
        for h in range(PARTS):
            partial_sums(1 - c, part, h)
            to_core[h].start()
        for h in range(PARTS):
            partial_sums(c, mine, h)
            to_core[h].wait_recv()
            mine[h] = mine[h] + from_core[h]
            to_pair[h].start()
        for i in range(EARLY, MIDDLE):
            halo(i).start()

        full = float(W)

        @pl.loop(0, series // LANES)
        def _(g):
            lanes = pl.ds(pl.multiple_of(g * LANES, LANES), LANES)
            for tile in range(time_rows // 8):
                keep[g, spread(tile, run, 8 * KEPT), :] = ret[
                    pl.ds(W + 8 * tile, 8), lanes
                ]

            def terms(q):
                r = keep[g, kept(q, 0), :]
                return [r, r * r]

            windows = [carried(t, back) for t in totals_of(terms, run)]
            for q in range(run):
                windows = slide(windows, terms(q), back)
                keep[g, kept(q, 1), :] = windows[0]
                keep[g, kept(q, 2), :] = windows[1] - windows[0] * (
                    windows[0] * (1.0 / full)
                )

        place_in = lax.broadcasted_iota(jnp.int32, (8, LANES), 0)
        for q in range(edge_run):
            seen = (place_in - edge_back) * edge_run + q + 1 + block * time_rows
            steps = jnp.minimum(jnp.maximum(seen, 1), W).astype(jnp.float32)
            edge_steps[0, eight(q), :] = 1.0 / steps
            edge_steps[1, eight(q), :] = ridge_rate * steps

        own = pl.ds(pl.multiple_of(c * half, half), half)
        share = [
            remote(
                means.at[own, columns(h)],
                means.at[own, columns(h)],
                ex_send.at[2, h],
                ex_recv.at[2, h],
                core,
            )
            for h in range(PARTS)
        ]
        counts = []
        for h in range(PARTS):
            to_pair[h].wait_recv()
            both = mine[h] + from_pair[h]
            counts.append(jnp.maximum(both[half : half + 1], 1.0))
            means[own, columns(h)] = both[:half] * (1.0 / counts[h])
            share[h].start()
        counts = jnp.concatenate(counts, axis=1)
        for h in range(PARTS):
            share[h].wait_recv()

        low = pl.multiple_of(c * tail, tail)
        pm_rows = prior.at[pl.ds(low, tail)]
        pm_on = remote(
            means.at[pl.ds(time_rows - W + low, tail)],
            pm_rows,
            pm_send.at[0],
            pm_recv.at[0],
            following,
        )
        pm_on.start()
        for i in range(MIDDLE, chunks):
            halo(i).start()

        for j in range(SECTORS // LANES):
            lanes = pl.ds(j * LANES, LANES)
            for tile in range(time_rows // 8):
                spreader[j, spread(tile, run), :] = means[eight(tile), lanes]
            for k, value in enumerate(split2(spreader[j])):
                mean_parts[k, :, lanes] = value

        def gathered(parts, i):
            hot = table[:, pl.ds(pl.multiple_of(i * CHUNK, CHUNK), CHUNK)]
            return nn(parts[0], hot) + nn(parts[1], hot)

        def interior(i):
            for s in range(GROUPS):
                g = i * GROUPS + s
                lanes = pl.ds(pl.multiple_of(g * LANES, LANES), LANES)
                inner = pl.ds(s * LANES, LANES)

                def terms(q):
                    f = fac[i, eight(q), inner]
                    return [f, f * f, keep[g, kept(q, 0), :] * f]

                windows = [carried(t, back) for t in totals_of(terms, run)]
                total = jnp.zeros((8, LANES), jnp.float32)
                for q in range(run):
                    windows = slide(windows, terms(q), back)
                    mean_fac = windows[0] * (1.0 / full)
                    cff = windows[1] - windows[0] * mean_fac
                    crf = windows[2] - keep[g, kept(q, 1), :] * mean_fac
                    value = (
                        keep[g, kept(q, 2), :] - crf * crf / (cff + ridge_rate * full)
                    ) * (1.0 / full)
                    total = total + value
                    work[s, eight(q), :] = (1.0 - shrink_weight) * value
                col[:, lanes] = jnp.where(place_in >= back, total, 0.0)
                for tile in range(W // 8, time_rows // 8):
                    var[eight(tile), lanes] = work[s, spread(tile, run), :]

        @pl.loop(0, chunks // BATCH)
        def _(i):
            for b in range(BATCH):
                fac[i * BATCH + b] = gathered(mean_parts, i * BATCH + b)

        pl.loop(0, chunks - LAST)(interior)
        pm_on.wait_recv()
        pm_share = remote(pm_rows, pm_rows, pm_send.at[1], pm_recv.at[1], core)
        pm_share.start()
        pl.loop(chunks - LAST, chunks)(interior)
        pm_share.wait_recv()
        started = block > 0

        for j in range(SECTORS // LANES):
            lanes = pl.ds(j * LANES, LANES)
            for tile in range(edge // 8):
                if tile < W // 8:
                    value = jnp.where(started, prior[eight(tile), lanes], 0.0)
                else:
                    value = means[eight(tile - W // 8), lanes]
                spreader[j, spread(tile, edge_run), :] = value
            for k, value in enumerate(split2(spreader[j, :edge, :])):
                edge_parts[k, :, lanes] = value

        @pl.loop(0, chunks // BATCH)
        def _(i):
            for b in range(BATCH):
                fac_edge[i * BATCH + b] = gathered(edge_parts, i * BATCH + b)

        late = place_in >= edge_back

        def boundary(i):
            halo(i).wait_recv()
            for s in range(GROUPS):
                lanes = pl.ds(pl.multiple_of(i * CHUNK + s * LANES, LANES), LANES)
                inner = pl.ds(s * LANES, LANES)
                for tile in range(edge // 8):
                    value = ret[eight(tile), lanes]
                    if tile < W // 8:
                        value = jnp.where(started, value, 0.0)
                    ret_edge[s, spread(tile, edge_run), :] = value

                def terms(q):
                    f = fac_edge[i, eight(q), inner]
                    r = ret_edge[s, eight(q), :]
                    return [r, r * r, f, f * f, r * f]

                windows = [carried(t, edge_back) for t in totals_of(terms, edge_run)]
                total = jnp.zeros((8, LANES), jnp.float32)
                for q in range(edge_run):
                    windows = slide(windows, terms(q), edge_back)
                    inv = edge_steps[0, eight(q), :]
                    s_r, s_rr, s_f, s_ff, s_rf = windows
                    mean_fac = s_f * inv
                    cff = s_ff - s_f * mean_fac
                    crf = s_rf - s_r * mean_fac
                    value = (
                        (s_rr - s_r * (s_r * inv))
                        - crf * crf / (cff + edge_steps[1, eight(q), :])
                    ) * inv
                    total = total + value
                    work[s, eight(q), :] = (1.0 - shrink_weight) * value
                col[:, lanes] += jnp.where(late, total, 0.0)
                for tile in range(W // 8, edge // 8):
                    var[eight(tile - W // 8), lanes] = work[s, spread(tile, edge_run), :]

        def sector_sums(first, last):
            cols = pl.ds(first * CHUNK, (last - first) * CHUNK)
            got = nt(jnp.concatenate(split3(col[:, cols]), axis=0), table[:, cols])
            return got[0:8] + got[8:16] + got[16:24]

        pl.loop(0, chunks - LAST)(boundary)
        sums[...] = sector_sums(0, chunks - LAST)
        pl.loop(chunks - LAST, chunks)(boundary)
        sums[...] += sector_sums(chunks - LAST, chunks)

        def exchange(buf, peer_of, send, recv, count, total):
            buf[0] = jnp.broadcast_to(total, (8, SECTORS))
            copies = [
                remote(
                    buf.at[0, pl.ds(0, 1)],
                    buf.at[d, pl.ds(0, 1)],
                    send.at[d],
                    recv.at[d],
                    peer_of(d),
                )
                for d in range(1, count)
            ]
            for copy in copies:
                copy.start()
            for copy in copies:
                copy.wait_recv()
            total = buf[0, 0:1]
            for d in range(1, count):
                total = total + buf[d, 0:1]
            return total, copies

        total = jnp.sum(sums[...], axis=0, keepdims=True)
        total, x_copies = exchange(gx, x_peer, gx_send, gx_recv, 8, total)
        total, y_copies = exchange(gy, y_peer, gy_send, gy_recv, n_y, total)
        total, z_copies = exchange(gz, z_peer, gz_send, gz_recv, n_z, total)

        all_steps = float(time_rows * n_blocks)
        sector_mean = total / (all_steps * counts)
        parts = split3(jnp.broadcast_to(shrink_weight * sector_mean, (8, SECTORS)))
        got = nn(jnp.concatenate(parts, axis=0), table[...])
        pooled_ref[...] = got[0:1] + got[8:9] + got[16:17]

        for i in range(chunks):
            halo(i).wait_send()
        for copy in (*to_core, *to_pair, *share, pm_on, pm_share):
            copy.wait_send()
        for copy in x_copies + y_copies + z_copies:
            copy.wait_send()

    return kernel


def last_add(var, pooled, out, held, sems):
    rows = var.shape[0] // 4
    copies = []
    for i in range(4):
        block = pl.ds(i * rows, rows)
        held[block] = var[block] + pooled[...]
        copies.append(pltpu.make_async_copy(held.at[block], out.at[block], sems.at[i]))
        copies[-1].start()
    for copy in copies:
        copy.wait()


def solution(mesh):
    series_axis = mesh.shape["series"]
    torus = Mesh(mesh.devices.reshape(8, 8, 2, series_axis // 2, 2), AXES)
    sizes = dict(torus.shape)
    n_y, n_z = sizes["y"], sizes["z"]

    def local(returns, sector):
        time_rows, series = returns.shape
        half = time_rows // 2
        chunks = series // CHUNK
        groups = series // LANES
        f32, bf16 = jnp.float32, jnp.bfloat16
        dma = pltpu.SemaphoreType.DMA
        vmem = pltpu.VMEM
        variance, pooled = pl.pallas_call(
            make_kernel(sizes, time_rows, series),
            name="rolling",
            out_shape=(
                vmem((time_rows, series), f32),
                vmem((1, series), f32),
            ),
            in_specs=[pl.BlockSpec(memory_space=pltpu.HBM)] * 2,
            out_specs=(
                pl.BlockSpec(memory_space=pltpu.VMEM),
                pl.BlockSpec(memory_space=pltpu.VMEM),
            ),
            scratch_shapes=[
                vmem((1, series), jnp.int32),
                vmem((time_rows + W, series), f32),
                vmem((groups, KEPT * time_rows, LANES), f32),
                vmem((SECTORS, series), bf16),
                vmem((PARTS, half + COUNT_ROWS, SECTORS // PARTS), f32),
                vmem((PARTS, half + COUNT_ROWS, SECTORS // PARTS), f32),
                vmem((PARTS, half + COUNT_ROWS, SECTORS // PARTS), f32),
                vmem((PARTS, half + COUNT_ROWS, SECTORS // PARTS), f32),
                vmem((time_rows, SECTORS), f32),
                vmem((W, SECTORS), f32),
                vmem((SECTORS // LANES, time_rows, LANES), f32),
                vmem((2, time_rows, SECTORS), bf16),
                vmem((2, 2 * W, SECTORS), bf16),
                vmem((chunks, time_rows, CHUNK), f32),
                vmem((chunks, 2 * W, CHUNK), f32),
                vmem((GROUPS, time_rows, LANES), f32),
                vmem((GROUPS, 2 * W, LANES), f32),
                vmem((2, 2 * W, LANES), f32),
                vmem((8, series), f32),
                vmem((8, SECTORS), f32),
                vmem((8, 8, SECTORS), f32),
                vmem((n_y, 8, SECTORS), f32),
                vmem((n_z, 8, SECTORS), f32),
                dma((3,)),
                dma((chunks,)),
                dma((chunks,)),
                dma((3, PARTS)),
                dma((3, PARTS)),
                dma((2,)),
                dma((2,)),
                dma((8,)),
                dma((8,)),
                dma((n_y,)),
                dma((n_y,)),
                dma((n_z,)),
                dma((n_z,)),
            ],
            compiler_params=pltpu.CompilerParams(
                collective_id=0, has_side_effects=True, vmem_limit_bytes=48 * 2**20
            ),
        )(
            pltpu.with_memory_space_constraint(returns, pltpu.HBM),
            pltpu.with_memory_space_constraint(sector[None, :], pltpu.HBM),
        )
        return pl.pallas_call(
            last_add,
            name="last_add",
            out_shape=jax.ShapeDtypeStruct((time_rows, series), f32),
            in_specs=[pl.BlockSpec(memory_space=pltpu.VMEM)] * 2,
            out_specs=pl.BlockSpec(memory_space=pl.ANY),
            scratch_shapes=[vmem((time_rows, series), f32), dma((4,))],
            compiler_params=pltpu.CompilerParams(vmem_limit_bytes=8 * 2**20),
        )(variance, pooled)

    return jax.shard_map(
        local,
        mesh=torus,
        in_specs=(P(("y", "z", "xh"), ("xl", "c")), P(("xl", "c"))),
        out_specs=P(("y", "z", "xh"), ("xl", "c")),
        check_vma=False,
    )
```

```python
import jax
import jax.numpy as jnp
from jax import lax
from jax.experimental import pallas as pl
from jax.experimental.pallas import tpu as pltpu
from jax.sharding import Mesh
from jax.sharding import PartitionSpec as P

W = 64
SECTORS = 512
AXES = ("y", "z", "xh", "xl", "c")
MESH_IDS = pl.DeviceIdType.MESH

ridge_rate = 0.05
shrink_weight = 0.3

LANES = 128
COUNT_ROWS = 8
CHUNK = 256
GROUPS = CHUNK // LANES
DEPTH = 512
KEPT = 3
PARTS = 2
EARLY = 2
MIDDLE = 3
BATCH = 4
LAST = 2


def split3(value):
    hi = value.astype(jnp.bfloat16)
    rest = value - hi.astype(jnp.float32)
    mid = rest.astype(jnp.bfloat16)
    lo = (rest - mid.astype(jnp.float32)).astype(jnp.bfloat16)
    return hi, mid, lo


def split2(value):
    hi = value.astype(jnp.bfloat16)
    return hi, (value - hi.astype(jnp.float32)).astype(jnp.bfloat16)


def nn(a, b):
    return jnp.dot(a, b, preferred_element_type=jnp.float32)


def nt(a, b):
    return lax.dot_general(
        a, b, (((1,), (1,)), ((), ())), preferred_element_type=jnp.float32
    )


def eight(q):
    return pl.ds(8 * q, 8)


def spread(tile, run, pitch=8):
    per = run // 8
    return pl.ds(8 * pitch * (tile % per) + tile // per, 8, stride=pitch)


def kept(q, k):
    return pl.ds(KEPT * 8 * q + 8 * k, 8)


def carried(total, back):
    out = pltpu.roll(total, 1, 0)
    for j in range(2, back + 1):
        out = out + pltpu.roll(total, j, 0)
    return out


def totals_of(terms, run):
    total = terms(0)
    for q in range(1, run):
        total = [a + b for a, b in zip(total, terms(q))]
    return total


def slide(windows, terms, back):
    return [s + (v - pltpu.roll(v, back, 0)) for s, v in zip(windows, terms)]


def remote(src, dst, send, recv, device):
    return pltpu.make_async_remote_copy(
        src_ref=src,
        dst_ref=dst,
        send_sem=send,
        recv_sem=recv,
        device_id=device,
        device_id_type=MESH_IDS,
    )


def make_kernel(sizes, time_rows, series):
    n_y, n_z = sizes["y"], sizes["z"]
    half = time_rows // 2
    chunks = series // CHUNK
    tail = W // 2
    body = half - tail
    run = time_rows // 8
    back = W // run
    edge = 2 * W
    edge_run = edge // 8
    edge_back = W // edge_run

    def kernel(
        ret_hbm,
        sector_hbm,
        var,
        pooled_ref,
        sector,
        ret,
        keep,
        table,
        part,
        mine,
        from_core,
        from_pair,
        means,
        prior,
        spreader,
        mean_parts,
        edge_parts,
        fac,
        fac_edge,
        work,
        ret_edge,
        edge_steps,
        col,
        sums,
        gx,
        gy,
        gz,
        load_sem,
        halo_send,
        halo_recv,
        ex_send,
        ex_recv,
        pm_send,
        pm_recv,
        gx_send,
        gx_recv,
        gy_send,
        gy_recv,
        gz_send,
        gz_recv,
    ):
        loads = [
            pltpu.make_async_copy(sector_hbm, sector, load_sem.at[2]),
            pltpu.make_async_copy(
                ret_hbm.at[time_rows - W :], ret.at[time_rows:], load_sem.at[0]
            ),
            pltpu.make_async_copy(
                ret_hbm.at[: time_rows - W], ret.at[W:time_rows], load_sem.at[1]
            ),
        ]
        for load in loads:
            load.start()

        y, z = lax.axis_index("y"), lax.axis_index("z")
        xh, xl, c = lax.axis_index("xh"), lax.axis_index("xl"), lax.axis_index("c")
        block = (y * n_z + z) * 2 + xh
        n_blocks = n_y * n_z * 2

        def place(b):
            b = lax.rem(b + n_blocks, n_blocks)
            return {"y": b // (2 * n_z), "z": lax.rem(b // 2, n_z), "xh": lax.rem(b, 2)}

        following, previous = place(block + 1), place(block - 1)
        core = {"c": 1 - c}
        pair = {"xl": 1 - xl}

        def x_peer(d):
            p = lax.rem(xh * 4 + xl * 2 + c + d, 8)
            return {"xh": p // 4, "xl": lax.rem(p // 2, 2), "c": lax.rem(p, 2)}

        def y_peer(d):
            return {"y": lax.rem(y + d, n_y)}

        def z_peer(d):
            return {"z": lax.rem(z + d, n_z)}

        peers = [following, previous]
        peers += [x_peer(d) for d in range(1, 8)]
        peers += [y_peer(d) for d in range(1, n_y)]
        peers += [z_peer(d) for d in range(1, n_z)]
        barrier = pltpu.get_barrier_semaphore()
        for peer in peers:
            pl.semaphore_signal(barrier, inc=1, device_id=peer, device_id_type=MESH_IDS)

        loads[0].wait()

        @pl.loop(0, chunks)
        def _(i):
            at = pl.multiple_of(i * CHUNK, CHUNK)
            labels = lax.broadcasted_iota(jnp.int32, (SECTORS, CHUNK), 0)
            hit = labels == sector[:, pl.ds(at, CHUNK)]
            table[:, pl.ds(at, CHUNK)] = hit.astype(jnp.float32).astype(jnp.bfloat16)

        loads[1].wait()
        pl.semaphore_wait(barrier, len(peers))

        def halo(i):
            at = pl.multiple_of(i * CHUNK, CHUNK)
            return remote(
                ret.at[time_rows:, pl.ds(at, CHUNK)],
                ret.at[:W, pl.ds(at, CHUNK)],
                halo_send.at[i],
                halo_recv.at[i],
                following,
            )

        for i in range(EARLY):
            halo(i).start()
        loads[2].wait()

        def columns(h):
            return pl.ds(h * (SECTORS // PARTS), SECTORS // PARTS)

        def partial_sums(which, into, h):
            first = pl.multiple_of(W + which * body, tail)
            last = pl.multiple_of(time_rows + which * tail, tail)
            ones = jnp.ones((2 * COUNT_ROWS, DEPTH), jnp.bfloat16)
            got = None
            for at in range(0, series, DEPTH):
                cols = pl.ds(at, DEPTH)
                rows = jnp.concatenate(
                    [ret[pl.ds(first, body), cols], ret[pl.ds(last, tail), cols]], axis=0
                )
                hi, lo = split2(rows)
                more = nt(jnp.concatenate([hi, lo, ones], axis=0), table[columns(h), cols])
                got = more if got is None else got + more
            into[h, :half] = got[:half] + got[half : 2 * half]
            into[h, half:] = got[2 * half : 2 * half + COUNT_ROWS]

        to_core = [
            remote(part.at[h], from_core.at[h], ex_send.at[0, h], ex_recv.at[0, h], core)
            for h in range(PARTS)
        ]
        to_pair = [
            remote(mine.at[h], from_pair.at[h], ex_send.at[1, h], ex_recv.at[1, h], pair)
            for h in range(PARTS)
        ]
        for h in range(PARTS):
            partial_sums(1 - c, part, h)
            to_core[h].start()
        for h in range(PARTS):
            partial_sums(c, mine, h)
            to_core[h].wait_recv()
            mine[h] = mine[h] + from_core[h]
            to_pair[h].start()
        full = float(W)

        @pl.loop(0, series // LANES)
        def _(g):
            lanes = pl.ds(pl.multiple_of(g * LANES, LANES), LANES)
            for tile in range(time_rows // 8):
                keep[g, spread(tile, run, 8 * KEPT), :] = ret[
                    pl.ds(W + 8 * tile, 8), lanes
                ]

            def terms(q):
                r = keep[g, kept(q, 0), :]
                return [r, r * r]

            windows = [carried(t, back) for t in totals_of(terms, run)]
            for q in range(run):
                windows = slide(windows, terms(q), back)
                keep[g, kept(q, 1), :] = windows[0]
                keep[g, kept(q, 2), :] = windows[1] - windows[0] * (
                    windows[0] * (1.0 / full)
                )

        place_in = lax.broadcasted_iota(jnp.int32, (8, LANES), 0)
        for q in range(edge_run):
            seen = (place_in - edge_back) * edge_run + q + 1 + block * time_rows
            steps = jnp.minimum(jnp.maximum(seen, 1), W).astype(jnp.float32)
            edge_steps[0, eight(q), :] = 1.0 / steps
            edge_steps[1, eight(q), :] = ridge_rate * steps

        low = pl.multiple_of(c * tail, tail)
        owned = (
            pl.ds(pl.multiple_of(c * body, tail), body),
            pl.ds(pl.multiple_of(time_rows - W + c * tail, tail), tail),
        )
        pm_rows = prior.at[pl.ds(low, tail)]
        share = [
            [
                remote(
                    means.at[rows, columns(h)],
                    means.at[rows, columns(h)],
                    ex_send.at[2 + k, h],
                    ex_recv.at[2 + k, h],
                    core,
                )
                for k, rows in enumerate(owned)
            ]
            for h in range(PARTS)
        ]
        pm_on = [
            remote(
                means.at[owned[1], columns(h)],
                prior.at[pl.ds(low, tail), columns(h)],
                pm_send.at[h],
                pm_recv.at[h],
                following,
            )
            for h in range(PARTS)
        ]
        counts = []
        for h in range(PARTS):
            to_pair[h].wait_recv()
            both = mine[h] + from_pair[h]
            counts.append(jnp.maximum(both[half : half + 1], 1.0))
            scaled = both[:half] * (1.0 / counts[h])
            means[owned[1], columns(h)] = scaled[body:]
            means[owned[0], columns(h)] = scaled[:body]
            pm_on[h].start()
            for copy in share[h]:
                copy.start()
            for i in (range(EARLY, MIDDLE), range(MIDDLE, chunks))[h]:
                halo(i).start()
        counts = jnp.concatenate(counts, axis=1)
        for h in range(PARTS):
            for copy in share[h]:
                copy.wait_recv()

        for j in range(SECTORS // LANES):
            lanes = pl.ds(j * LANES, LANES)
            for tile in range(time_rows // 8):
                spreader[j, spread(tile, run), :] = means[eight(tile), lanes]
            for k, value in enumerate(split2(spreader[j])):
                mean_parts[k, :, lanes] = value

        def gathered(parts, i):
            hot = table[:, pl.ds(pl.multiple_of(i * CHUNK, CHUNK), CHUNK)]
            return nn(parts[0], hot) + nn(parts[1], hot)

        def interior(i):
            for s in range(GROUPS):
                g = i * GROUPS + s
                lanes = pl.ds(pl.multiple_of(g * LANES, LANES), LANES)
                inner = pl.ds(s * LANES, LANES)

                def terms(q):
                    f = fac[i, eight(q), inner]
                    return [f, f * f, keep[g, kept(q, 0), :] * f]

                windows = [carried(t, back) for t in totals_of(terms, run)]
                total = jnp.zeros((8, LANES), jnp.float32)
                for q in range(run):
                    windows = slide(windows, terms(q), back)
                    mean_fac = windows[0] * (1.0 / full)
                    cff = windows[1] - windows[0] * mean_fac
                    crf = windows[2] - keep[g, kept(q, 1), :] * mean_fac
                    value = (
                        keep[g, kept(q, 2), :] - crf * crf / (cff + ridge_rate * full)
                    ) * (1.0 / full)
                    total = total + value
                    work[s, eight(q), :] = (1.0 - shrink_weight) * value
                col[:, lanes] = jnp.where(place_in >= back, total, 0.0)
                for tile in range(W // 8, time_rows // 8):
                    var[eight(tile), lanes] = work[s, spread(tile, run), :]

        @pl.loop(0, chunks // BATCH)
        def _(i):
            for b in range(BATCH):
                fac[i * BATCH + b] = gathered(mean_parts, i * BATCH + b)

        pl.loop(0, chunks // 2)(interior)
        for copy in pm_on:
            copy.wait_recv()
        pm_share = remote(pm_rows, pm_rows, pm_send.at[2], pm_recv.at[2], core)
        pm_share.start()
        pl.loop(chunks // 2, chunks)(interior)
        pm_share.wait_recv()
        started = block > 0

        for j in range(SECTORS // LANES):
            lanes = pl.ds(j * LANES, LANES)
            for tile in range(edge // 8):
                if tile < W // 8:
                    value = jnp.where(started, prior[eight(tile), lanes], 0.0)
                else:
                    value = means[eight(tile - W // 8), lanes]
                spreader[j, spread(tile, edge_run), :] = value
            for k, value in enumerate(split2(spreader[j, :edge, :])):
                edge_parts[k, :, lanes] = value

        @pl.loop(0, chunks // BATCH)
        def _(i):
            for b in range(BATCH):
                fac_edge[i * BATCH + b] = gathered(edge_parts, i * BATCH + b)

        late = place_in >= edge_back

        def boundary(i):
            halo(i).wait_recv()
            for s in range(GROUPS):
                lanes = pl.ds(pl.multiple_of(i * CHUNK + s * LANES, LANES), LANES)
                inner = pl.ds(s * LANES, LANES)
                for tile in range(edge // 8):
                    value = ret[eight(tile), lanes]
                    if tile < W // 8:
                        value = jnp.where(started, value, 0.0)
                    ret_edge[s, spread(tile, edge_run), :] = value

                def terms(q):
                    f = fac_edge[i, eight(q), inner]
                    r = ret_edge[s, eight(q), :]
                    return [r, r * r, f, f * f, r * f]

                windows = [carried(t, edge_back) for t in totals_of(terms, edge_run)]
                total = jnp.zeros((8, LANES), jnp.float32)
                for q in range(edge_run):
                    windows = slide(windows, terms(q), edge_back)
                    inv = edge_steps[0, eight(q), :]
                    s_r, s_rr, s_f, s_ff, s_rf = windows
                    mean_fac = s_f * inv
                    cff = s_ff - s_f * mean_fac
                    crf = s_rf - s_r * mean_fac
                    value = (
                        (s_rr - s_r * (s_r * inv))
                        - crf * crf / (cff + edge_steps[1, eight(q), :])
                    ) * inv
                    total = total + value
                    work[s, eight(q), :] = (1.0 - shrink_weight) * value
                col[:, lanes] += jnp.where(late, total, 0.0)
                for tile in range(W // 8, edge // 8):
                    var[eight(tile - W // 8), lanes] = work[s, spread(tile, edge_run), :]

        def sector_sums(first, last):
            cols = pl.ds(first * CHUNK, (last - first) * CHUNK)
            got = nt(jnp.concatenate(split3(col[:, cols]), axis=0), table[:, cols])
            return got[0:8] + got[8:16] + got[16:24]

        pl.loop(0, chunks - LAST)(boundary)
        sums[...] = sector_sums(0, chunks - LAST)
        pl.loop(chunks - LAST, chunks)(boundary)
        sums[...] += sector_sums(chunks - LAST, chunks)

        def exchange(buf, peer_of, send, recv, count, total):
            buf[0] = jnp.broadcast_to(total, (8, SECTORS))
            copies = [
                remote(
                    buf.at[0, pl.ds(0, 1)],
                    buf.at[d, pl.ds(0, 1)],
                    send.at[d],
                    recv.at[d],
                    peer_of(d),
                )
                for d in range(1, count)
            ]
            for copy in copies:
                copy.start()
            for copy in copies:
                copy.wait_recv()
            total = buf[0, 0:1]
            for d in range(1, count):
                total = total + buf[d, 0:1]
            return total, copies

        total = jnp.sum(sums[...], axis=0, keepdims=True)
        total, x_copies = exchange(gx, x_peer, gx_send, gx_recv, 8, total)
        total, y_copies = exchange(gy, y_peer, gy_send, gy_recv, n_y, total)
        total, z_copies = exchange(gz, z_peer, gz_send, gz_recv, n_z, total)

        all_steps = float(time_rows * n_blocks)
        sector_mean = total / (all_steps * counts)
        parts = split3(jnp.broadcast_to(shrink_weight * sector_mean, (8, SECTORS)))
        got = nn(jnp.concatenate(parts, axis=0), table[...])
        pooled_ref[...] = got[0:1] + got[8:9] + got[16:17]

        for i in range(chunks):
            halo(i).wait_send()
        for copy in (*to_core, *to_pair, *share[0], *share[1], *pm_on, pm_share):
            copy.wait_send()
        for copy in x_copies + y_copies + z_copies:
            copy.wait_send()

    return kernel


def last_add(var, pooled, out, held, sems):
    rows = var.shape[0] // 4
    copies = []
    for i in range(4):
        block = pl.ds(i * rows, rows)
        held[block] = var[block] + pooled[...]
        copies.append(pltpu.make_async_copy(held.at[block], out.at[block], sems.at[i]))
        copies[-1].start()
    for copy in copies:
        copy.wait()


def solution(mesh):
    series_axis = mesh.shape["series"]
    torus = Mesh(mesh.devices.reshape(8, 8, 2, series_axis // 2, 2), AXES)
    sizes = dict(torus.shape)
    n_y, n_z = sizes["y"], sizes["z"]

    def local(returns, sector):
        time_rows, series = returns.shape
        half = time_rows // 2
        chunks = series // CHUNK
        groups = series // LANES
        f32, bf16 = jnp.float32, jnp.bfloat16
        dma = pltpu.SemaphoreType.DMA
        vmem = pltpu.VMEM
        variance, pooled = pl.pallas_call(
            make_kernel(sizes, time_rows, series),
            name="rolling",
            out_shape=(
                vmem((time_rows, series), f32),
                vmem((1, series), f32),
            ),
            in_specs=[pl.BlockSpec(memory_space=pltpu.HBM)] * 2,
            out_specs=(
                pl.BlockSpec(memory_space=pltpu.VMEM),
                pl.BlockSpec(memory_space=pltpu.VMEM),
            ),
            scratch_shapes=[
                vmem((1, series), jnp.int32),
                vmem((time_rows + W, series), f32),
                vmem((groups, KEPT * time_rows, LANES), f32),
                vmem((SECTORS, series), bf16),
                vmem((PARTS, half + COUNT_ROWS, SECTORS // PARTS), f32),
                vmem((PARTS, half + COUNT_ROWS, SECTORS // PARTS), f32),
                vmem((PARTS, half + COUNT_ROWS, SECTORS // PARTS), f32),
                vmem((PARTS, half + COUNT_ROWS, SECTORS // PARTS), f32),
                vmem((time_rows, SECTORS), f32),
                vmem((W, SECTORS), f32),
                vmem((SECTORS // LANES, time_rows, LANES), f32),
                vmem((2, time_rows, SECTORS), bf16),
                vmem((2, 2 * W, SECTORS), bf16),
                vmem((chunks, time_rows, CHUNK), f32),
                vmem((chunks, 2 * W, CHUNK), f32),
                vmem((GROUPS, time_rows, LANES), f32),
                vmem((GROUPS, 2 * W, LANES), f32),
                vmem((2, 2 * W, LANES), f32),
                vmem((8, series), f32),
                vmem((8, SECTORS), f32),
                vmem((8, 8, SECTORS), f32),
                vmem((n_y, 8, SECTORS), f32),
                vmem((n_z, 8, SECTORS), f32),
                dma((3,)),
                dma((chunks,)),
                dma((chunks,)),
                dma((4, PARTS)),
                dma((4, PARTS)),
                dma((3,)),
                dma((3,)),
                dma((8,)),
                dma((8,)),
                dma((n_y,)),
                dma((n_y,)),
                dma((n_z,)),
                dma((n_z,)),
            ],
            compiler_params=pltpu.CompilerParams(
                collective_id=0, has_side_effects=True, vmem_limit_bytes=48 * 2**20
            ),
        )(
            pltpu.with_memory_space_constraint(returns, pltpu.HBM),
            pltpu.with_memory_space_constraint(sector[None, :], pltpu.HBM),
        )
        return pl.pallas_call(
            last_add,
            name="last_add",
            out_shape=jax.ShapeDtypeStruct((time_rows, series), f32),
            in_specs=[pl.BlockSpec(memory_space=pltpu.VMEM)] * 2,
            out_specs=pl.BlockSpec(memory_space=pl.ANY),
            scratch_shapes=[vmem((time_rows, series), f32), dma((4,))],
            compiler_params=pltpu.CompilerParams(vmem_limit_bytes=8 * 2**20),
        )(variance, pooled)

    return jax.shard_map(
        local,
        mesh=torus,
        in_specs=(P(("y", "z", "xh"), ("xl", "c")), P(("xl", "c"))),
        out_specs=P(("y", "z", "xh"), ("xl", "c")),
        check_vma=False,
    )
```

```python
import jax
import jax.numpy as jnp
from jax import lax
from jax.experimental import pallas as pl
from jax.experimental.pallas import tpu as pltpu
from jax.sharding import Mesh
from jax.sharding import PartitionSpec as P

W = 64
SECTORS = 512
AXES = ("y", "z", "xh", "xl", "c")
MESH_IDS = pl.DeviceIdType.MESH

ridge_rate = 0.05
shrink_weight = 0.3

LANES = 128
COUNT_ROWS = 8
CHUNK = 256
GROUPS = CHUNK // LANES
DEPTH = 512
KEPT = 3
PARTS = 2
EARLY = 2
MIDDLE = 4
BATCH = 4
LAST = 2


def split3(value):
    hi = value.astype(jnp.bfloat16)
    rest = value - hi.astype(jnp.float32)
    mid = rest.astype(jnp.bfloat16)
    lo = (rest - mid.astype(jnp.float32)).astype(jnp.bfloat16)
    return hi, mid, lo


def split2(value):
    hi = value.astype(jnp.bfloat16)
    return hi, (value - hi.astype(jnp.float32)).astype(jnp.bfloat16)


def nn(a, b):
    return jnp.dot(a, b, preferred_element_type=jnp.float32)


def nt(a, b):
    return lax.dot_general(
        a, b, (((1,), (1,)), ((), ())), preferred_element_type=jnp.float32
    )


def eight(q):
    return pl.ds(8 * q, 8)


def spread(tile, run, pitch=8):
    per = run // 8
    return pl.ds(8 * pitch * (tile % per) + tile // per, 8, stride=pitch)


def kept(q, k):
    return pl.ds(KEPT * 8 * q + 8 * k, 8)


def carried(total, back):
    out = pltpu.roll(total, 1, 0)
    for j in range(2, back + 1):
        out = out + pltpu.roll(total, j, 0)
    return out


def totals_of(terms, run):
    total = terms(0)
    for q in range(1, run):
        total = [a + b for a, b in zip(total, terms(q))]
    return total


def slide(windows, terms, back):
    return [s + (v - pltpu.roll(v, back, 0)) for s, v in zip(windows, terms)]


def remote(src, dst, send, recv, device):
    return pltpu.make_async_remote_copy(
        src_ref=src,
        dst_ref=dst,
        send_sem=send,
        recv_sem=recv,
        device_id=device,
        device_id_type=MESH_IDS,
    )


def make_kernel(sizes, time_rows, series):
    n_y, n_z = sizes["y"], sizes["z"]
    half = time_rows // 2
    chunks = series // CHUNK
    tail = W // 2
    body = half - tail
    run = time_rows // 8
    back = W // run
    edge = 2 * W
    edge_run = edge // 8
    edge_back = W // edge_run

    def kernel(
        ret_hbm,
        sector_hbm,
        var,
        pooled_ref,
        sector,
        ret,
        keep,
        table,
        part,
        mine,
        from_core,
        from_pair,
        means,
        prior,
        spreader,
        mean_parts,
        edge_parts,
        fac,
        fac_edge,
        work,
        ret_edge,
        edge_steps,
        col,
        sums,
        gx,
        gy,
        gz,
        load_sem,
        halo_send,
        halo_recv,
        ex_send,
        ex_recv,
        pm_send,
        pm_recv,
        gx_send,
        gx_recv,
        gy_send,
        gy_recv,
        gz_send,
        gz_recv,
    ):
        loads = [
            pltpu.make_async_copy(sector_hbm, sector, load_sem.at[2]),
            pltpu.make_async_copy(
                ret_hbm.at[time_rows - W :], ret.at[time_rows:], load_sem.at[0]
            ),
            pltpu.make_async_copy(
                ret_hbm.at[: time_rows - W], ret.at[W:time_rows], load_sem.at[1]
            ),
        ]
        for load in loads:
            load.start()

        y, z = lax.axis_index("y"), lax.axis_index("z")
        xh, xl, c = lax.axis_index("xh"), lax.axis_index("xl"), lax.axis_index("c")
        block = (y * n_z + z) * 2 + xh
        n_blocks = n_y * n_z * 2

        def place(b):
            b = lax.rem(b + n_blocks, n_blocks)
            return {"y": b // (2 * n_z), "z": lax.rem(b // 2, n_z), "xh": lax.rem(b, 2)}

        following, previous = place(block + 1), place(block - 1)
        core = {"c": 1 - c}
        pair = {"xl": 1 - xl}

        def x_peer(d):
            p = lax.rem(xh * 4 + xl * 2 + c + d, 8)
            return {"xh": p // 4, "xl": lax.rem(p // 2, 2), "c": lax.rem(p, 2)}

        def y_peer(d):
            return {"y": lax.rem(y + d, n_y)}

        def z_peer(d):
            return {"z": lax.rem(z + d, n_z)}

        peers = [following, previous]
        peers += [x_peer(d) for d in range(1, 8)]
        peers += [y_peer(d) for d in range(1, n_y)]
        peers += [z_peer(d) for d in range(1, n_z)]
        barrier = pltpu.get_barrier_semaphore()
        for peer in peers:
            pl.semaphore_signal(barrier, inc=1, device_id=peer, device_id_type=MESH_IDS)

        loads[0].wait()

        @pl.loop(0, chunks)
        def _(i):
            at = pl.multiple_of(i * CHUNK, CHUNK)
            labels = lax.broadcasted_iota(jnp.int32, (SECTORS, CHUNK), 0)
            hit = labels == sector[:, pl.ds(at, CHUNK)]
            table[:, pl.ds(at, CHUNK)] = hit.astype(jnp.float32).astype(jnp.bfloat16)

        loads[1].wait()
        pl.semaphore_wait(barrier, len(peers))

        def halo(i):
            at = pl.multiple_of(i * CHUNK, CHUNK)
            return remote(
                ret.at[time_rows:, pl.ds(at, CHUNK)],
                ret.at[:W, pl.ds(at, CHUNK)],
                halo_send.at[i],
                halo_recv.at[i],
                following,
            )

        for i in range(EARLY):
            halo(i).start()
        loads[2].wait()

        def columns(h):
            return pl.ds(h * (SECTORS // PARTS), SECTORS // PARTS)

        def partial_sums(which, into, h):
            first = pl.multiple_of(W + which * body, tail)
            last = pl.multiple_of(time_rows + which * tail, tail)
            ones = jnp.ones((2 * COUNT_ROWS, DEPTH), jnp.bfloat16)
            got = None
            for at in range(0, series, DEPTH):
                cols = pl.ds(at, DEPTH)
                rows = jnp.concatenate(
                    [ret[pl.ds(first, body), cols], ret[pl.ds(last, tail), cols]], axis=0
                )
                hi, lo = split2(rows)
                more = nt(jnp.concatenate([hi, lo, ones], axis=0), table[columns(h), cols])
                got = more if got is None else got + more
            into[h, :half] = got[:half] + got[half : 2 * half]
            into[h, half:] = got[2 * half : 2 * half + COUNT_ROWS]

        to_core = [
            remote(part.at[h], from_core.at[h], ex_send.at[0, h], ex_recv.at[0, h], core)
            for h in range(PARTS)
        ]
        to_pair = [
            remote(mine.at[h], from_pair.at[h], ex_send.at[1, h], ex_recv.at[1, h], pair)
            for h in range(PARTS)
        ]
        for h in range(PARTS):
            partial_sums(1 - c, part, h)
            to_core[h].start()
        for h in range(PARTS):
            partial_sums(c, mine, h)
            to_core[h].wait_recv()
            mine[h] = mine[h] + from_core[h]
            to_pair[h].start()
        for i in range(EARLY, MIDDLE):
            halo(i).start()
        full = float(W)

        @pl.loop(0, series // LANES)
        def _(g):
            lanes = pl.ds(pl.multiple_of(g * LANES, LANES), LANES)
            for tile in range(time_rows // 8):
                keep[g, spread(tile, run, 8 * KEPT), :] = ret[
                    pl.ds(W + 8 * tile, 8), lanes
                ]

            def terms(q):
                r = keep[g, kept(q, 0), :]
                return [r, r * r]

            windows = [carried(t, back) for t in totals_of(terms, run)]
            for q in range(run):
                windows = slide(windows, terms(q), back)
                keep[g, kept(q, 1), :] = windows[0]
                keep[g, kept(q, 2), :] = windows[1] - windows[0] * (
                    windows[0] * (1.0 / full)
                )

        place_in = lax.broadcasted_iota(jnp.int32, (8, LANES), 0)
        for q in range(edge_run):
            seen = (place_in - edge_back) * edge_run + q + 1 + block * time_rows
            steps = jnp.minimum(jnp.maximum(seen, 1), W).astype(jnp.float32)
            edge_steps[0, eight(q), :] = 1.0 / steps
            edge_steps[1, eight(q), :] = ridge_rate * steps

        low = pl.multiple_of(c * tail, tail)
        owned = (
            pl.ds(pl.multiple_of(c * body, tail), body),
            pl.ds(pl.multiple_of(time_rows - W + c * tail, tail), tail),
        )
        pm_rows = prior.at[pl.ds(low, tail)]
        share = [
            [
                remote(
                    means.at[rows, columns(h)],
                    means.at[rows, columns(h)],
                    ex_send.at[2 + k, h],
                    ex_recv.at[2 + k, h],
                    core,
                )
                for k, rows in enumerate(owned)
            ]
            for h in range(PARTS)
        ]
        pm_on = [
            remote(
                means.at[owned[1], columns(h)],
                prior.at[pl.ds(low, tail), columns(h)],
                pm_send.at[h],
                pm_recv.at[h],
                following,
            )
            for h in range(PARTS)
        ]
        counts = []
        for h in range(PARTS):
            to_pair[h].wait_recv()
            both = mine[h] + from_pair[h]
            counts.append(jnp.maximum(both[half : half + 1], 1.0))
            scaled = both[:half] * (1.0 / counts[h])
            means[owned[1], columns(h)] = scaled[body:]
            means[owned[0], columns(h)] = scaled[:body]
            for copy in share[h]:
                copy.start()
            pm_on[h].start()
        counts = jnp.concatenate(counts, axis=1)
        for h in range(PARTS):
            for copy in share[h]:
                copy.wait_recv()
        for i in range(MIDDLE, chunks):
            halo(i).start()

        for j in range(SECTORS // LANES):
            lanes = pl.ds(j * LANES, LANES)
            for tile in range(time_rows // 8):
                spreader[j, spread(tile, run), :] = means[eight(tile), lanes]
            for k, value in enumerate(split2(spreader[j])):
                mean_parts[k, :, lanes] = value

        def gathered(parts, i):
            hot = table[:, pl.ds(pl.multiple_of(i * CHUNK, CHUNK), CHUNK)]
            return nn(parts[0], hot) + nn(parts[1], hot)

        def interior(i):
            for s in range(GROUPS):
                g = i * GROUPS + s
                lanes = pl.ds(pl.multiple_of(g * LANES, LANES), LANES)
                inner = pl.ds(s * LANES, LANES)

                def terms(q):
                    f = fac[i, eight(q), inner]
                    return [f, f * f, keep[g, kept(q, 0), :] * f]

                windows = [carried(t, back) for t in totals_of(terms, run)]
                total = jnp.zeros((8, LANES), jnp.float32)
                for q in range(run):
                    windows = slide(windows, terms(q), back)
                    mean_fac = windows[0] * (1.0 / full)
                    cff = windows[1] - windows[0] * mean_fac
                    crf = windows[2] - keep[g, kept(q, 1), :] * mean_fac
                    value = (
                        keep[g, kept(q, 2), :] - crf * crf / (cff + ridge_rate * full)
                    ) * (1.0 / full)
                    total = total + value
                    work[s, eight(q), :] = (1.0 - shrink_weight) * value
                col[:, lanes] = jnp.where(place_in >= back, total, 0.0)
                for tile in range(W // 8, time_rows // 8):
                    var[eight(tile), lanes] = work[s, spread(tile, run), :]

        @pl.loop(0, chunks // BATCH)
        def _(i):
            for b in range(BATCH):
                fac[i * BATCH + b] = gathered(mean_parts, i * BATCH + b)

        pl.loop(0, chunks // 2)(interior)
        for copy in pm_on:
            copy.wait_recv()
        pm_share = remote(pm_rows, pm_rows, pm_send.at[2], pm_recv.at[2], core)
        pm_share.start()
        pl.loop(chunks // 2, chunks)(interior)
        pm_share.wait_recv()
        started = block > 0

        for j in range(SECTORS // LANES):
            lanes = pl.ds(j * LANES, LANES)
            for tile in range(edge // 8):
                if tile < W // 8:
                    value = jnp.where(started, prior[eight(tile), lanes], 0.0)
                else:
                    value = means[eight(tile - W // 8), lanes]
                spreader[j, spread(tile, edge_run), :] = value
            for k, value in enumerate(split2(spreader[j, :edge, :])):
                edge_parts[k, :, lanes] = value

        @pl.loop(0, chunks // BATCH)
        def _(i):
            for b in range(BATCH):
                fac_edge[i * BATCH + b] = gathered(edge_parts, i * BATCH + b)

        late = place_in >= edge_back

        def boundary(i):
            halo(i).wait_recv()
            for s in range(GROUPS):
                lanes = pl.ds(pl.multiple_of(i * CHUNK + s * LANES, LANES), LANES)
                inner = pl.ds(s * LANES, LANES)
                for tile in range(edge // 8):
                    value = ret[eight(tile), lanes]
                    if tile < W // 8:
                        value = jnp.where(started, value, 0.0)
                    ret_edge[s, spread(tile, edge_run), :] = value

                def terms(q):
                    f = fac_edge[i, eight(q), inner]
                    r = ret_edge[s, eight(q), :]
                    return [r, r * r, f, f * f, r * f]

                windows = [carried(t, edge_back) for t in totals_of(terms, edge_run)]
                total = jnp.zeros((8, LANES), jnp.float32)
                for q in range(edge_run):
                    windows = slide(windows, terms(q), edge_back)
                    inv = edge_steps[0, eight(q), :]
                    s_r, s_rr, s_f, s_ff, s_rf = windows
                    mean_fac = s_f * inv
                    cff = s_ff - s_f * mean_fac
                    crf = s_rf - s_r * mean_fac
                    value = (
                        (s_rr - s_r * (s_r * inv))
                        - crf * crf / (cff + edge_steps[1, eight(q), :])
                    ) * inv
                    total = total + value
                    work[s, eight(q), :] = (1.0 - shrink_weight) * value
                col[:, lanes] += jnp.where(late, total, 0.0)
                for tile in range(W // 8, edge // 8):
                    var[eight(tile - W // 8), lanes] = work[s, spread(tile, edge_run), :]

        def sector_sums(first, last):
            cols = pl.ds(first * CHUNK, (last - first) * CHUNK)
            got = nt(jnp.concatenate(split3(col[:, cols]), axis=0), table[:, cols])
            return got[0:8] + got[8:16] + got[16:24]

        pl.loop(0, chunks - LAST)(boundary)
        sums[...] = sector_sums(0, chunks - LAST)
        pl.loop(chunks - LAST, chunks)(boundary)
        sums[...] += sector_sums(chunks - LAST, chunks)

        def exchange(buf, peer_of, send, recv, count, total):
            buf[0] = jnp.broadcast_to(total, (8, SECTORS))
            copies = [
                remote(
                    buf.at[0, pl.ds(0, 1)],
                    buf.at[d, pl.ds(0, 1)],
                    send.at[d],
                    recv.at[d],
                    peer_of(d),
                )
                for d in range(1, count)
            ]
            for copy in copies:
                copy.start()
            for copy in copies:
                copy.wait_recv()
            total = buf[0, 0:1]
            for d in range(1, count):
                total = total + buf[d, 0:1]
            return total, copies

        total = jnp.sum(sums[...], axis=0, keepdims=True)
        total, x_copies = exchange(gx, x_peer, gx_send, gx_recv, 8, total)
        total, y_copies = exchange(gy, y_peer, gy_send, gy_recv, n_y, total)
        total, z_copies = exchange(gz, z_peer, gz_send, gz_recv, n_z, total)

        all_steps = float(time_rows * n_blocks)
        sector_mean = total / (all_steps * counts)
        parts = split3(jnp.broadcast_to(shrink_weight * sector_mean, (8, SECTORS)))
        got = nn(jnp.concatenate(parts, axis=0), table[...])
        pooled_ref[...] = got[0:1] + got[8:9] + got[16:17]

        for i in range(chunks):
            halo(i).wait_send()
        for copy in (*to_core, *to_pair, *share[0], *share[1], *pm_on, pm_share):
            copy.wait_send()
        for copy in x_copies + y_copies + z_copies:
            copy.wait_send()

    return kernel


def last_add(var, pooled, out, held, sems):
    rows = var.shape[0] // 4
    copies = []
    for i in range(4):
        block = pl.ds(i * rows, rows)
        held[block] = var[block] + pooled[...]
        copies.append(pltpu.make_async_copy(held.at[block], out.at[block], sems.at[i]))
        copies[-1].start()
    for copy in copies:
        copy.wait()


def solution(mesh):
    series_axis = mesh.shape["series"]
    torus = Mesh(mesh.devices.reshape(8, 8, 2, series_axis // 2, 2), AXES)
    sizes = dict(torus.shape)
    n_y, n_z = sizes["y"], sizes["z"]

    def local(returns, sector):
        time_rows, series = returns.shape
        half = time_rows // 2
        chunks = series // CHUNK
        groups = series // LANES
        f32, bf16 = jnp.float32, jnp.bfloat16
        dma = pltpu.SemaphoreType.DMA
        vmem = pltpu.VMEM
        variance, pooled = pl.pallas_call(
            make_kernel(sizes, time_rows, series),
            name="rolling",
            out_shape=(
                vmem((time_rows, series), f32),
                vmem((1, series), f32),
            ),
            in_specs=[pl.BlockSpec(memory_space=pltpu.HBM)] * 2,
            out_specs=(
                pl.BlockSpec(memory_space=pltpu.VMEM),
                pl.BlockSpec(memory_space=pltpu.VMEM),
            ),
            scratch_shapes=[
                vmem((1, series), jnp.int32),
                vmem((time_rows + W, series), f32),
                vmem((groups, KEPT * time_rows, LANES), f32),
                vmem((SECTORS, series), bf16),
                vmem((PARTS, half + COUNT_ROWS, SECTORS // PARTS), f32),
                vmem((PARTS, half + COUNT_ROWS, SECTORS // PARTS), f32),
                vmem((PARTS, half + COUNT_ROWS, SECTORS // PARTS), f32),
                vmem((PARTS, half + COUNT_ROWS, SECTORS // PARTS), f32),
                vmem((time_rows, SECTORS), f32),
                vmem((W, SECTORS), f32),
                vmem((SECTORS // LANES, time_rows, LANES), f32),
                vmem((2, time_rows, SECTORS), bf16),
                vmem((2, 2 * W, SECTORS), bf16),
                vmem((chunks, time_rows, CHUNK), f32),
                vmem((chunks, 2 * W, CHUNK), f32),
                vmem((GROUPS, time_rows, LANES), f32),
                vmem((GROUPS, 2 * W, LANES), f32),
                vmem((2, 2 * W, LANES), f32),
                vmem((8, series), f32),
                vmem((8, SECTORS), f32),
                vmem((8, 8, SECTORS), f32),
                vmem((n_y, 8, SECTORS), f32),
                vmem((n_z, 8, SECTORS), f32),
                dma((3,)),
                dma((chunks,)),
                dma((chunks,)),
                dma((4, PARTS)),
                dma((4, PARTS)),
                dma((3,)),
                dma((3,)),
                dma((8,)),
                dma((8,)),
                dma((n_y,)),
                dma((n_y,)),
                dma((n_z,)),
                dma((n_z,)),
            ],
            compiler_params=pltpu.CompilerParams(
                collective_id=0, has_side_effects=True, vmem_limit_bytes=48 * 2**20
            ),
        )(
            pltpu.with_memory_space_constraint(returns, pltpu.HBM),
            pltpu.with_memory_space_constraint(sector[None, :], pltpu.HBM),
        )
        return pl.pallas_call(
            last_add,
            name="last_add",
            out_shape=jax.ShapeDtypeStruct((time_rows, series), f32),
            in_specs=[pl.BlockSpec(memory_space=pltpu.VMEM)] * 2,
            out_specs=pl.BlockSpec(memory_space=pl.ANY),
            scratch_shapes=[vmem((time_rows, series), f32), dma((4,))],
            compiler_params=pltpu.CompilerParams(vmem_limit_bytes=8 * 2**20),
        )(variance, pooled)

    return jax.shard_map(
        local,
        mesh=torus,
        in_specs=(P(("y", "z", "xh"), ("xl", "c")), P(("xl", "c"))),
        out_specs=P(("y", "z", "xh"), ("xl", "c")),
        check_vma=False,
    )
```
